128 devices in a mesh: gz: 4 (over x), gy: 4 (over z), gx: 8 (over y, core).
Axes of the slice: x: 4, y: 4, z: 4, core: 2. Of those that a mesh axis runs over, the one named last changes fastest.
Arguments:
- spins: float32 [2, 64, 192, 1024], P(None, 'gz', 'gy', 'gx'), may hold values from -6 to 6
- kicks: float32 [2, 2, 64, 192, 1024], P(None, None, 'gz', 'gy', 'gx'), may hold values from -6 to 6
- stiffness: float32 [64, 192, 1024], P('gz', 'gy', 'gx'), may hold values from 0.1 to 11, as said below
Outputs:
- final_spins: float32 [2, 64, 192, 1024], P(None, 'gz', 'gy', 'gx')
- section_energy: float32 [16], replicated
The draws below stay inside these ranges and needn't reach their ends.
Inputs may be any that keep to these rules, and one draw needn't show every extreme that they name: `stiffness`: positive coupling strengths.
All inputs are finite; a program needn't handle non-finite values.
Results may differ from the reference program's by a relative error of at most 0.0001.
Values sent between devices are 32-bit elements; how exact they have to be, the bound alone decides.
A program may use at most 128 MiB of HBM per device.

```python
import jax
import jax.numpy as jnp
from jax import lax

SWEEPS = 2
NZ = 64
NY = 192
NX = 1024


def draw_stiffness(key, part):
    shape = (NZ, NY, NX)
    zpos = lax.broadcasted_iota(jnp.float32, shape, 0) / NZ
    ypos = lax.broadcasted_iota(jnp.float32, shape, 1) / NY
    xpos = lax.broadcasted_iota(jnp.float32, shape, 2) / NX
    base = jnp.exp(jax.random.uniform(key, shape, jnp.float32, jnp.log(0.1), jnp.log(0.4)))
    ramp = jnp.exp(jnp.log(3.0) * (zpos + ypos + xpos))
    return (base * ramp).astype(jnp.float32)


def block_scale(rng, dims, shards, low, largest):
    gain = 1.0
    for axis_at, blocks in shards:
        heights = jax.random.uniform(jax.random.fold_in(jax.random.fold_in(rng, 6), axis_at), (blocks,), jnp.float32, low / len(shards), largest / len(shards))
        gain = gain * jnp.repeat(jnp.exp(heights), dims[axis_at] // blocks).reshape((-1,) + (1,) * (len(dims) - 1 - axis_at))
    return gain


def scatter_about(stream_key, extent, scale, reach, shards=(), kind=jnp.bfloat16):
    result = scale * jax.random.normal(stream_key, extent, jnp.float32)
    if shards:
        result = result * block_scale(stream_key, extent, shards, -0.22, 0.18)
    return jnp.clip(result, -reach, reach).astype(kind)


def setup_inputs(seed: int = 0) -> dict:
    key_of = jax.random.split(jax.random.key(seed), 4)
    spins = scatter_about(key_of[0], (2, NZ, NY, NX), 1.0, 6.0, ((1, 4), (2, 4), (3, 8)), jnp.float32)
    kicks = scatter_about(key_of[1], (SWEEPS, 2, NZ, NY, NX), 1.0, 6.0, ((2, 4), (3, 4), (4, 8)), jnp.float32)
    stiffness = draw_stiffness(jax.random.fold_in(key_of[3], 71), 0)
    return {"spins": spins, "kicks": kicks, "stiffness": stiffness}


def neighbour_sum(field):
    total = jnp.zeros(field.shape, jnp.float32)
    for axis in range(3):
        for offset in (1, -1):
            total = total + jnp.roll(field, offset, axis)
    return total

def reference(spins, kicks, stiffness):
    shape = stiffness.shape
    zpar = lax.broadcasted_iota(jnp.int32, shape, 0) % 2
    ypar = lax.broadcasted_iota(jnp.int32, shape, 1) % 2
    xpar = lax.broadcasted_iota(jnp.int32, shape, 2) % 2
    colour = 4 * zpar + 2 * ypar + xpar
    first = spins[0]
    second = spins[1]
    sites = jnp.float32(NZ * NY * NX // 8)
    records = []
    for sweep in range(SWEEPS):
        for section in range(8):
            local_a = stiffness * neighbour_sum(first) + kicks[sweep, 0]
            local_b = stiffness * neighbour_sum(second) + kicks[sweep, 1]
            scale = 1.0 / jnp.sqrt(1.0 + local_a * local_a + local_b * local_b)
            new_a = local_a * scale
            new_b = local_b * scale
            member = colour == section
            first = jnp.where(member, new_a, first)
            second = jnp.where(member, new_b, second)
            energy = jnp.sum(jnp.where(member, new_a * local_a + new_b * local_b, jnp.float32(0.0)))
            records.append(-energy / sites)
    return (jnp.stack([first, second]), jnp.stack(records).astype(jnp.float32))
```

```python
import functools

import jax
import jax.numpy as jnp
from jax import lax
from jax.experimental import pallas as pl
from jax.experimental.pallas import tpu as pltpu
from jax.sharding import PartitionSpec as P

MESH = pl.DeviceIdType.MESH
F32 = jnp.float32
NZ, NY, NX = 16, 48, 128
PITCH = 56
ROWS = 19 * PITCH
TILES = 7

MESSAGES = {
    "Z": ((-1, 0, 0), 256, 112),
    "z": ((1, 0, 0), 96, 96),
    "Y": ((0, -1, 0), 96, 48),
    "y": ((0, 1, 0), 32, 32),
    "ZY": ((-1, -1, 0), 24, 24),
    "Zy": ((-1, 1, 0), 8, 8),
    "zY": ((1, -1, 0), 8, 8),
    "X": ((0, 0, -1), 40, 16),
    "XZ": ((-1, 0, -1), 40, 16),
    "XY": ((0, -1, -1), 40, 16),
    "XZY": ((-1, -1, -1), 40, 16),
    "Xz": ((1, 0, -1), 16, 16),
    "Xy": ((0, 1, -1), 16, 16),
    "XZy": ((-1, 1, -1), 16, 16),
    "XzY": ((1, -1, -1), 16, 16),
    "x": ((0, 0, 1), 16, 16),
    "xZ": ((-1, 0, 1), 16, 16),
    "xY": ((0, -1, 1), 16, 16),
    "xZY": ((-1, -1, 1), 16, 16),
}
NAMES = list(MESSAGES)
COUNT = len(NAMES)


def offsets(round_index):
    start, table = 0, {}
    for name in NAMES:
        size = MESSAGES[name][1 + round_index]
        table[name] = (start, size)
        start += size
    return table, start


TABLE_A, SIZE_A = offsets(0)
TABLE_B, SIZE_B = offsets(1)


def row(z, y):
    return (z + 1) * PITCH + y


def roll(v, shift, axis=1):
    shift = shift % v.shape[axis]
    return v if shift == 0 else pltpu.roll(v, shift, axis)


def kernel(dims, spins, kicks, stiff, out, energy_out, S, J, K, XH, send_a, recv_a, send_b, recv_b, EN, ebuf, erow,
           load_sem, out_sem, sa_sem, ra_sem, sb_sem, rb_sem, es_sem, er_sem):
    nz, ny, nx = dims
    total = nz * ny * nx
    me = (lax.axis_index("gz"), lax.axis_index("gy"), lax.axis_index("gx"))

    def device(step):
        return tuple(lax.rem(m + (d % n), n) for m, d, n in zip(me, step, dims))

    lane = lax.broadcasted_iota(jnp.int32, (8, 128), 1)
    sub = lax.broadcasted_iota(jnp.int32, (8, 128), 0)
    zi = (lane * 9363) >> 16
    tile = lane - zi * 7

    def load(z, which):
        dst = pl.ds(pl.multiple_of((z + 1) * PITCH, 8), NY)
        if which == 0:
            return pltpu.make_async_copy(spins.at[:, z], S.at[:, dst, :], load_sem.at[0, z])
        if which == 1:
            return pltpu.make_async_copy(stiff.at[z], J.at[dst, :], load_sem.at[1, z])
        w = which - 2
        return pltpu.make_async_copy(kicks.at[w, :, z], K.at[pl.ds(2 * w, 2), dst, :], load_sem.at[which, z])

    def each(f):
        def step(z, carry):
            f(z)
            return carry

        lax.fori_loop(0, NZ, step, 0)

    for which in range(4):
        each(lambda z, which=which: load(z, which).start())

    barrier = pltpu.get_barrier_semaphore()
    steps = [MESSAGES[name][0] for name in NAMES]
    steps += [(0, 0, d) for d in range(2, nx - 1)]
    for s in steps:
        pl.semaphore_signal(barrier, inc=1, device_id=device(tuple(-d for d in s)), device_id_type=MESH)

    for which in range(3):
        each(lambda z, which=which: load(z, which).wait())

    zero_plane = jnp.zeros((PITCH, 128), F32)
    for c in range(2):
        S[c, pl.ds(18 * PITCH, PITCH), :] = zero_plane
        S[c, pl.ds(row(0, 49), NZ, stride=PITCH), :] = jnp.zeros((NZ, 128), F32)
        S[c, pl.ds(row(16, 49), 1), :] = jnp.zeros((1, 128), F32)

    lane3 = lane - ((lane * 21846) >> 16) * 3
    group = [((lane - r + 1) * 21846) >> 16 for r in range(3)]
    own_tiles = [(z + 1) * TILES + t for z in range(NZ) for t in range(6)]

    def pack_spins():
        cols = []
        for c in range(2):
            acc = [jnp.zeros((8, 128), F32) for _ in range(3)]
            for q in own_tiles:
                r = q % 3
                v = roll(S[c, pl.ds(8 * q, 8), :], q)
                acc[r] = jnp.where(group[r] == q // 3, v, acc[r])

            def pick(shift):
                a = [roll(v, shift) for v in acc]
                return jnp.where(lane3 == 0, a[0], jnp.where(lane3 == 1, a[1], a[2]))

            cols.append((pick(0), pick(-1), pick(1)))
        return [[cols[c][k] for c in range(2)] for k in range(3)]

    def pack_first(read):
        acc = jnp.zeros((8, 128), F32)
        for q in own_tiles:
            acc = jnp.where(lane == q, roll(read(8 * q), q), acc)
        return acc

    def zplus(v):
        return roll(v, -7)

    def yplus(v):
        return roll(v, -1, 0)

    def copies(send, recv, table, ssem, rsem):
        result = {}
        for i, name in enumerate(NAMES):
            start, size = table[name]
            part = pl.ds(start, size)
            result[name] = pltpu.make_async_remote_copy(
                src_ref=send.at[part, :],
                dst_ref=recv.at[part, :],
                send_sem=ssem.at[i],
                recv_sem=rsem.at[i],
                device_id=device(MESSAGES[name][0]),
                device_id_type=MESH,
            )
        return result

    def put(send, table, name, at, value):
        send[pl.ds(table[name][0] + at, value.shape[0]), :] = value

    def get(recv, table, name, at, size=8):
        return recv[pl.ds(table[name][0] + at, size), :]

    copies_a = copies(send_a, recv_a, TABLE_A, sa_sem, ra_sem)
    copies_b = copies(send_b, recv_b, TABLE_B, sb_sem, rb_sem)

    def build(send, table, w):
        first = w == 0
        n = 5 if first else 2
        J0 = J[pl.ds(row(0, 0), NY), :]
        for c in range(2):
            kc = K[2 * w + c, pl.ds(row(0, 0), NY), :] + J0 * S[c, pl.ds(row(1, 0), NY), :]
            put(send, table, "Z", (n - 2 + c) * NY, kc)
            if first:
                put(send, table, "Z", c * NY, S[c, pl.ds(row(0, 0), NY), :])
            put(send, table, "z", c * NY, S[c, pl.ds(row(15, 0), NY), :])
        if first:
            put(send, table, "Z", 2 * NY, J0)
        rows0 = pl.ds(row(0, 0), NZ, stride=PITCH)
        rows1 = pl.ds(row(0, 1), NZ, stride=PITCH)
        rows47 = pl.ds(row(0, 47), NZ, stride=PITCH)
        Jy = J[rows0, :]
        for c in range(2):
            kc = K[2 * w + c, rows0, :] + Jy * S[c, rows1, :]
            put(send, table, "Y", (n - 2 + c) * NZ, kc)
            if first:
                put(send, table, "Y", c * NZ, S[c, rows0, :])
            put(send, table, "y", c * NZ, S[c, rows47, :])
        if first:
            put(send, table, "Y", 2 * NZ, Jy)
        at = pl.ds(row(0, 0), 1)
        for c in range(2):
            kc = K[2 * w + c, at, :] + J[at, :] * (S[c, pl.ds(row(1, 0), 1), :] + S[c, pl.ds(row(0, 1), 1), :])
            put(send, table, "ZY", n - 2 + c, kc)
            if first:
                put(send, table, "ZY", c, S[c, at, :])
            put(send, table, "Zy", c, S[c, pl.ds(row(0, 47), 1), :])
            put(send, table, "zY", c, S[c, pl.ds(row(15, 0), 1), :])
        if first:
            put(send, table, "ZY", 2, J[at, :])

    def build_columns(send, table, w, PJ, PK):
        first = w == 0
        n = 5 if first else 2
        PS, PT, PR = pack_spins()
        for c in range(2):
            zs, ys = zplus(PS[c]), yplus(PS[c])
            sums = {"X": PT[c], "XZ": PT[c] + zs, "XY": PT[c] + ys, "XZY": PT[c] + zs + ys}
            for name, value in sums.items():
                put(send, table, name, (n - 2 + c) * 8, PK[c] + PJ * value)
                if first:
                    put(send, table, name, c * 8, PS[c])
            for name in ("Xz", "Xy", "XZy", "XzY"):
                put(send, table, name, c * 8, PS[c])
            for name in ("x", "xZ", "xY", "xZY"):
                put(send, table, name, c * 8, PR[c])
            put(send, table, "Z", n * NY + c * 8, PR[c])
            put(send, table, "Y", n * NZ + c * 8, PR[c])
            put(send, table, "ZY", 8 + c * 8, PR[c])
        if first:
            for name in ("X", "XZ", "XY", "XZY"):
                put(send, table, name, 16, PJ)
        return PR

    def merge_faces(recv, table, w):
        first = w == 0
        n = 5 if first else 2
        plane = pl.ds(row(16, 0), NY)
        rows48 = pl.ds(row(0, 48), NZ, stride=PITCH)
        at = pl.ds(row(16, 48), 1)
        for c in range(2):
            K[2 * w + c, plane, :] = get(recv, table, "Z", (n - 2 + c) * NY, NY)
            K[2 * w + c, rows48, :] = get(recv, table, "Y", (n - 2 + c) * NZ, NZ)
            K[2 * w + c, at, :] = get(recv, table, "ZY", n - 2 + c, 1)
            if first:
                S[c, plane, :] = get(recv, table, "Z", c * NY, NY)
                S[c, rows48, :] = get(recv, table, "Y", c * NZ, NZ)
                S[c, at, :] = get(recv, table, "ZY", c, 1)
            S[c, pl.ds(row(-1, 0), NY), :] = get(recv, table, "z", c * NY, NY)
            S[c, pl.ds(row(0, -1), NZ, stride=PITCH), :] = get(recv, table, "y", c * NZ, NZ)
            S[c, pl.ds(row(16, -1), 1), :] = get(recv, table, "Zy", c, 1)
            S[c, pl.ds(row(-1, 48), 1), :] = get(recv, table, "zY", c, 1)
        if first:
            J[plane, :] = get(recv, table, "Z", 2 * NY, NY)
            J[rows48, :] = get(recv, table, "Y", 2 * NZ, NZ)
            J[at, :] = get(recv, table, "ZY", 2, 1)

    at_z = (zi == 17) & (tile < 6)
    at_y = (tile == 6) & (sub == 0) & (zi >= 1) & (zi <= 16)
    at_zy = (zi == 17) & (tile == 6) & (sub == 0)
    at_zm = (zi == 0) & (tile < 6)
    at_ym = (tile == 6) & (sub == 7) & (zi <= 15)
    at_zym = (lane == 118) & (sub == 7)
    at_yzm = (lane == 6) & (sub == 0)

    def upper(base, vz, vy, vzy):
        base = jnp.where(at_z, roll(vz, 112), base)
        base = jnp.where(at_y, roll(vy, 6), base)
        return jnp.where(at_zy, roll(vzy, 118), base)

    def lower(base, recv, table, c):
        base = jnp.where(at_zm, roll(get(recv, table, "Xz", c * 8), -112), base)
        base = jnp.where(at_ym, roll(get(recv, table, "Xy", c * 8), -6), base)
        base = jnp.where(at_zym, roll(get(recv, table, "XZy", c * 8), 106), base)
        return jnp.where(at_yzm, roll(get(recv, table, "XzY", c * 8), -106), base)

    def merge_columns(recv, table, w, PR, ES, EJ):
        first = w == 0
        n = 5 if first else 2

        def ext(at):
            v = [get(recv, table, name, at) for name in ("X", "XZ", "XY", "XZY")]
            return upper(*v)

        EK = [ext((n - 2 + c) * 8) for c in range(2)]
        if first:
            ES = [ext(c * 8) for c in range(2)]
            EJ = ext(16)
        ES = [lower(ES[c], recv, table, c) for c in range(2)]
        HM = [upper(*[get(recv, table, name, c * 8) for name in ("x", "xZ", "xY", "xZY")]) for c in range(2)]
        PM = [
            upper(
                PR[c],
                get(recv, table, "Z", n * NY + c * 8),
                get(recv, table, "Y", n * NZ + c * 8),
                get(recv, table, "ZY", 8 + c * 8),
            )
            for c in range(2)
        ]
        return EK, ES, EJ, HM, PM

    def shift_up(v):
        v = roll(v, 1, 0)
        return jnp.where(sub == 0, roll(v, 1), v)

    def shift_down(v):
        v = roll(v, -1, 0)
        return jnp.where(sub == 7, roll(v, -1), v)

    inside = (zi >= 1) & (zi <= 17) & ((tile < 6) | (sub == 0))

    def update_column(EK, ES, EJ, PM):
        for zp in range(2):
            for yp in range(2):
                member = inside & ((zi & 1) == 1 - zp) & ((sub & 1) == yp)
                local = []
                for c in range(2):
                    v = ES[c]
                    above = jnp.where(lane < 17 * TILES, roll(v, -7), 0.0)
                    near = shift_up(v) + shift_down(v) + roll(v, 7) + above + PM[c]
                    local.append(EJ * near + EK[c])
                scale = lax.rsqrt(1.0 + (local[0] * local[0] + local[1] * local[1]))
                ES = [jnp.where(member, local[c] * scale, ES[c]) for c in range(2)]
        return ES

    def spread_columns(HM, ES):
        for c in range(2):
            e = roll(ES[c], -1)
            even = (lane & 1) == 0
            mixed = [jnp.where(even, HM[c], e), jnp.where(even, e, HM[c])]
            for q in range(TILES, 18 * TILES):
                XH[c, pl.ds(8 * q, 8), :] = roll(mixed[q % 2], -q)

    def update(w, base, n, stride, xp):
        def at(off):
            return pl.ds(base + off, n, stride=stride) if n > 1 else pl.ds(base + off, 1)

        lanes = lax.broadcasted_iota(jnp.int32, (n, 128), 1)
        member = (lanes & 1) == xp
        stiffness = J[at(0), :]
        local, centre = [], []
        for c in range(2):
            v = S[c, at(0), :]
            edge = XH[c, at(0), :]
            left, right = roll(v, 1), roll(v, -1)
            if xp == 0:
                left = jnp.where(lanes == 0, edge, left)
            else:
                right = jnp.where(lanes == 127, edge, right)
            near = (S[c, at(-1), :] + S[c, at(1), :]) + (S[c, at(-PITCH), :] + S[c, at(PITCH), :]) + (left + right)
            local.append(stiffness * near + K[2 * w + c, at(0), :])
            centre.append(v)
        q = local[0] * local[0] + local[1] * local[1]
        scale = lax.rsqrt(1.0 + q)
        for c in range(2):
            S[c, at(0), :] = jnp.where(member, local[c] * scale, centre[c])
        return q * scale

    def section(w, zp, yp, xp):
        energy = None
        for z in range(zp, NZ + 1 - zp, 2):
            e = update(w, row(z, yp), 24, 2, xp)
            if z < NZ:
                energy = e if energy is None else energy + e
        if yp == 0:
            update(w, row(zp, 48), 8, 2 * PITCH, xp)
            if zp == 0:
                update(w, row(16, 48), 1, 1, xp)
        energy = energy[0:8] + energy[8:16] + energy[16:24]
        t = 8 * w + 4 * zp + 2 * yp + xp
        EN[t] = jnp.where((lane & 1) == xp, energy, 0.0)

    build(send_a, TABLE_A, 0)
    PJ = pack_first(lambda r: J[pl.ds(r, 8), :])
    PK = [pack_first(lambda r, c=c: K[c, pl.ds(r, 8), :]) for c in range(2)]
    PR = build_columns(send_a, TABLE_A, 0, PJ, PK)
    pl.semaphore_wait(barrier, len(steps))
    for name in NAMES:
        copies_a[name].start()
    each(lambda z: load(z, 3).wait())
    PK = [pack_first(lambda r, c=c: K[2 + c, pl.ds(r, 8), :]) for c in range(2)]
    for name in NAMES:
        copies_a[name].wait_recv()
    merge_faces(recv_a, TABLE_A, 0)
    EK, ES, EJ, HM, PM = merge_columns(recv_a, TABLE_A, 0, PR, None, None)
    ES = update_column(EK, ES, EJ, PM)
    spread_columns(HM, ES)
    for t in range(8):
        section(0, t // 4, t // 2 % 2, t % 2)

    build(send_b, TABLE_B, 1)
    PR = build_columns(send_b, TABLE_B, 1, PJ, PK)
    for name in NAMES:
        copies_b[name].start()
    for name in NAMES:
        copies_a[name].wait_send()
    for name in NAMES:
        copies_b[name].wait_recv()
    merge_faces(recv_b, TABLE_B, 1)
    EK, ES, EJ, HM, PM = merge_columns(recv_b, TABLE_B, 1, PR, ES, EJ)
    ES = update_column(EK, ES, EJ, PM)
    spread_columns(HM, ES)
    for t in range(8):
        section(1, t // 4, t // 2 % 2, t % 2)

    def store(z):
        src = pl.ds(pl.multiple_of((z + 1) * PITCH, 8), NY)
        return pltpu.make_async_copy(S.at[:, src, :], out.at[:, z], out_sem.at[z])

    sums = jnp.sum(jnp.sum(EN[...], axis=1), axis=1, keepdims=True)
    diagonal = lax.broadcasted_iota(jnp.int32, (16, 128), 0) == lax.broadcasted_iota(jnp.int32, (16, 128), 1)
    mine = jnp.sum(jnp.where(diagonal, jnp.broadcast_to(sums, (16, 128)), 0.0), axis=0, keepdims=True)
    index = (me[0] * ny + me[1]) * nx + me[2]
    erow[0] = mine
    ebuf[index] = mine

    def share(i, carry):
        to = lax.rem(index + i, total)
        pltpu.make_async_remote_copy(
            src_ref=erow.at[0],
            dst_ref=ebuf.at[index],
            send_sem=es_sem,
            recv_sem=er_sem,
            device_id=(to // (ny * nx), lax.rem(to // nx, ny), lax.rem(to, nx)),
            device_id_type=MESH,
        ).start()
        return carry

    lax.fori_loop(1, total, share, 0)
    each(lambda z: store(z).start())
    for name in NAMES:
        copies_b[name].wait_send()
    rest = pl.ds(0, total - 1)
    done = pltpu.make_async_remote_copy(
        src_ref=ebuf.at[rest],
        dst_ref=ebuf.at[rest],
        send_sem=es_sem,
        recv_sem=er_sem,
        device_id=me,
        device_id_type=MESH,
    )
    done.wait_recv()
    whole = ebuf[0]
    for i in range(1, total):
        whole = whole + ebuf[i]
    sites = float(8 // 8 * (NZ * nz) * (NY * ny) * (NX * nx) // 8)
    energy_out[...] = -whole / sites
    done.wait_send()
    each(lambda z: store(z).wait())


def body(dims, spins, kicks, stiffness):
    hbm = pl.BlockSpec(memory_space=pl.ANY)
    total = dims[0] * dims[1] * dims[2]
    vmem, dma = pltpu.VMEM, pltpu.SemaphoreType.DMA
    final, energy = pl.pallas_call(
        functools.partial(kernel, dims),
        out_shape=(
            jax.ShapeDtypeStruct((2, NZ, NY, NX), F32),
            jax.ShapeDtypeStruct((1, 128), F32),
        ),
        in_specs=[hbm] * 3,
        out_specs=(hbm, pl.BlockSpec(memory_space=vmem)),
        scratch_shapes=[
            vmem((2, ROWS, 128), F32),
            vmem((ROWS, 128), F32),
            vmem((4, ROWS, 128), F32),
            vmem((2, ROWS, 128), F32),
            vmem((SIZE_A, 128), F32),
            vmem((SIZE_A, 128), F32),
            vmem((SIZE_B, 128), F32),
            vmem((SIZE_B, 128), F32),
            vmem((16, 8, 128), F32),
            vmem((total, 1, 128), F32),
            vmem((1, 1, 128), F32),
            dma((4, NZ)),
            dma((NZ,)),
            dma((COUNT,)),
            dma((COUNT,)),
            dma((COUNT,)),
            dma((COUNT,)),
            dma,
            dma,
        ],
        compiler_params=pltpu.CompilerParams(collective_id=0, has_side_effects=True),
    )(spins, kicks, stiffness)
    return final, energy[0, :16]


def solution(mesh):
    dims = tuple(mesh.shape[a] for a in ("gz", "gy", "gx"))
    return jax.shard_map(
        functools.partial(body, dims),
        mesh=mesh,
        in_specs=(P(None, "gz", "gy", "gx"), P(None, None, "gz", "gy", "gx"), P("gz", "gy", "gx")),
        out_specs=(P(None, "gz", "gy", "gx"), P()),
        check_vma=False,
    )
```

```python
import functools

import jax
import jax.numpy as jnp
from jax import lax
from jax.experimental import pallas as pl
from jax.experimental.pallas import tpu as pltpu
from jax.sharding import PartitionSpec as P

MESH = pl.DeviceIdType.MESH
F32 = jnp.float32
NZ, NY, NX = 16, 48, 128
PITCH = 56
ROWS = 19 * PITCH
TILES = 7

MESSAGES = {
    "XZY": ((-1, -1, -1), 8, 8),
    "XZy": ((-1, 1, -1), 8, 8),
    "XzY": ((1, -1, -1), 8, 8),
    "xZY": ((-1, -1, 1), 8, 8),
    "ZY": ((-1, -1, 0), 8, 8),
    "Zy": ((-1, 1, 0), 8, 8),
    "zY": ((1, -1, 0), 8, 8),
    "XZ": ((-1, 0, -1), 8, 8),
    "XY": ((0, -1, -1), 8, 8),
    "Xz": ((1, 0, -1), 8, 8),
    "Xy": ((0, 1, -1), 8, 8),
    "xZ": ((-1, 0, 1), 8, 8),
    "xY": ((0, -1, 1), 8, 8),
    "PZ": ((-1, 0, 0), 8, 8),
    "PY": ((0, -1, 0), 8, 8),
    "X": ((0, 0, -1), 40, 16),
    "x": ((0, 0, 1), 16, 16),
    "Z": ((-1, 0, 0), 240, 96),
    "z": ((1, 0, 0), 96, 96),
    "Y": ((0, -1, 0), 80, 32),
    "y": ((0, 1, 0), 32, 32),
}
NAMES = list(MESSAGES)
COUNT = len(NAMES)
FACES = ("Zy", "zY", "Z", "z", "Y", "y")
COLUMNS = [name for name in NAMES if name not in FACES]


def offsets(round_index):
    start, table = 0, {}
    for name in NAMES:
        size = MESSAGES[name][1 + round_index]
        table[name] = (start, size)
        start += size
    return table, start


TABLE_A, SIZE_A = offsets(0)
TABLE_B, SIZE_B = offsets(1)


def row(z, y):
    return (z + 1) * PITCH + y


def roll(v, shift, axis=1):
    shift = shift % v.shape[axis]
    return v if shift == 0 else pltpu.roll(v, shift, axis)


def kernel(dims, spins, kicks, stiff, out, energy_out, S, J, K, XH, send_a, recv_a, send_b, recv_b, EN, ebuf, erow,
           load_sem, sa_sem, ra_sem, sb_sem, rb_sem, es_sem, er_sem):
    nz, ny, nx = dims
    total = nz * ny * nx
    me = (lax.axis_index("gz"), lax.axis_index("gy"), lax.axis_index("gx"))

    def device(step):
        return tuple(lax.rem(m + (d % n), n) for m, d, n in zip(me, step, dims))

    lane = lax.broadcasted_iota(jnp.int32, (8, 128), 1)
    sub = lax.broadcasted_iota(jnp.int32, (8, 128), 0)
    zi = (lane * 9363) >> 16
    tile = lane - zi * 7

    def load(z, which):
        dst = pl.ds(pl.multiple_of((z + 1) * PITCH, 8), NY)
        if which == 0:
            return pltpu.make_async_copy(spins.at[:, z], S.at[:, dst, :], load_sem.at[0, z])
        if which == 1:
            return pltpu.make_async_copy(stiff.at[z], J.at[dst, :], load_sem.at[1, z])
        w = which - 2
        return pltpu.make_async_copy(kicks.at[w, :, z], K.at[pl.ds(2 * w, 2), dst, :], load_sem.at[which, z])

    def each(f):
        def step(z, carry):
            f(z)
            return carry

        lax.fori_loop(0, NZ, step, 0)

    for which in range(4):
        each(lambda z, which=which: load(z, which).start())

    barrier = pltpu.get_barrier_semaphore()
    steps = sorted({MESSAGES[name][0] for name in NAMES})
    steps += [(0, 0, d) for d in range(2, nx - 1)]
    for s in steps:
        pl.semaphore_signal(barrier, inc=1, device_id=device(tuple(-d for d in s)), device_id_type=MESH)

    for which in range(3):
        each(lambda z, which=which: load(z, which).wait())

    zero_plane = jnp.zeros((PITCH, 128), F32)
    for c in range(2):
        S[c, pl.ds(18 * PITCH, PITCH), :] = zero_plane
        S[c, pl.ds(row(0, 49), NZ, stride=PITCH), :] = jnp.zeros((NZ, 128), F32)
        S[c, pl.ds(row(16, 49), 1), :] = jnp.zeros((1, 128), F32)

    lane3 = lane - ((lane * 21846) >> 16) * 3
    group = [((lane - r + 1) * 21846) >> 16 for r in range(3)]
    own_tiles = [(z + 1) * TILES + t for z in range(NZ) for t in range(6)]

    def pack_spins():
        cols = []
        for c in range(2):
            acc = [jnp.zeros((8, 128), F32) for _ in range(3)]
            for q in own_tiles:
                r = q % 3
                v = roll(S[c, pl.ds(8 * q, 8), :], q)
                acc[r] = jnp.where(group[r] == q // 3, v, acc[r])

            def pick(shift):
                a = [roll(v, shift) for v in acc]
                return jnp.where(lane3 == 0, a[0], jnp.where(lane3 == 1, a[1], a[2]))

            cols.append((pick(0), pick(-1), pick(1)))
        return [[cols[c][k] for c in range(2)] for k in range(3)]

    def pack_first(read):
        acc = jnp.zeros((8, 128), F32)
        for q in own_tiles:
            acc = jnp.where(lane == q, roll(read(8 * q), q), acc)
        return acc

    def zplus(v):
        return roll(v, -7)

    def yplus(v):
        return roll(v, -1, 0)

    def copies(send, recv, table, ssem, rsem):
        result = {}
        for i, name in enumerate(NAMES):
            start, size = table[name]
            part = pl.ds(start, size)
            result[name] = pltpu.make_async_remote_copy(
                src_ref=send.at[part, :],
                dst_ref=recv.at[part, :],
                send_sem=ssem.at[i],
                recv_sem=rsem.at[i],
                device_id=device(MESSAGES[name][0]),
                device_id_type=MESH,
            )
        return result

    def put(send, table, name, at, value):
        send[pl.ds(table[name][0] + at, value.shape[0]), :] = value

    def get(recv, table, name, at, size=8):
        return recv[pl.ds(table[name][0] + at, size), :]

    copies_a = copies(send_a, recv_a, TABLE_A, sa_sem, ra_sem)
    copies_b = copies(send_b, recv_b, TABLE_B, sb_sem, rb_sem)

    def build(send, table, w):
        first = w == 0
        n = 5 if first else 2
        J0 = J[pl.ds(row(0, 0), NY), :]
        for c in range(2):
            kc = K[2 * w + c, pl.ds(row(0, 0), NY), :] + J0 * S[c, pl.ds(row(1, 0), NY), :]
            put(send, table, "Z", (n - 2 + c) * NY, kc)
            if first:
                put(send, table, "Z", c * NY, S[c, pl.ds(row(0, 0), NY), :])
            put(send, table, "z", c * NY, S[c, pl.ds(row(15, 0), NY), :])
        if first:
            put(send, table, "Z", 2 * NY, J0)
        rows0 = pl.ds(row(0, 0), NZ, stride=PITCH)
        rows1 = pl.ds(row(0, 1), NZ, stride=PITCH)
        rows47 = pl.ds(row(0, 47), NZ, stride=PITCH)
        Jy = J[rows0, :]
        for c in range(2):
            kc = K[2 * w + c, rows0, :] + Jy * S[c, rows1, :]
            put(send, table, "Y", (n - 2 + c) * NZ, kc)
            if first:
                put(send, table, "Y", c * NZ, S[c, rows0, :])
            put(send, table, "y", c * NZ, S[c, rows47, :])
        if first:
            put(send, table, "Y", 2 * NZ, Jy)
        at = pl.ds(row(0, 0), 1)
        for c in range(2):
            kc = K[2 * w + c, at, :] + J[at, :] * (S[c, pl.ds(row(1, 0), 1), :] + S[c, pl.ds(row(0, 1), 1), :])
            put(send, table, "ZY", n - 2 + c, kc)
            if first:
                put(send, table, "ZY", c, S[c, at, :])
            put(send, table, "Zy", c, S[c, pl.ds(row(0, 47), 1), :])
            put(send, table, "zY", c, S[c, pl.ds(row(15, 0), 1), :])
        if first:
            put(send, table, "ZY", 2, J[at, :])

    def by_lanes(values, shift=0):
        acc = values[0]
        for k in range(1, len(values)):
            acc = jnp.where((lane >> 4) == k, roll(values[k], 16 * k), acc)
        return acc

    def by_rows(values):
        acc = values[0]
        for k in range(1, len(values)):
            acc = jnp.where(sub == k, roll(values[k], k, 0), acc)
        return acc

    def build_columns(send, table, w, PJ, PK):
        first = w == 0
        PS, PT, PR = pack_spins()
        parts = {name: [] for name in ("X", "XZ", "XY", "XZY")}
        for c in range(2):
            zs, ys = zplus(PS[c]), yplus(PS[c])
            sums = {"X": PT[c], "XZ": PT[c] + zs, "XY": PT[c] + ys, "XZY": PT[c] + zs + ys}
            for name, value in sums.items():
                parts[name].append(PK[c] + PJ * value)
        if first:
            parts = {name: PS + [PJ] + value for name, value in parts.items()}
        put(send, table, "XZY", 0, by_rows(parts["XZY"]))
        put(send, table, "XZ", 0, by_lanes(parts["XZ"]))
        put(send, table, "XY", 0, by_rows(parts["XY"]))
        for k, value in enumerate(parts["X"]):
            put(send, table, "X", 8 * k, value)
        last = jnp.where(sub == 6, roll(PS[1], -1, 0), PS[0])
        put(send, table, "XZy", 0, last)
        put(send, table, "Xy", 0, last)
        put(send, table, "XzY", 0, by_rows(PS))
        put(send, table, "Xz", 0, jnp.where((lane >> 4) == 6, roll(PS[1], -16), PS[0]))
        rows, lanes = by_rows(PR), by_lanes(PR)
        for name in ("xZY", "xY", "PY"):
            put(send, table, name, 0, rows)
        for name in ("xZ", "PZ"):
            put(send, table, name, 0, lanes)
        put(send, table, "ZY", 5, rows[0:2])
        for c in range(2):
            put(send, table, "x", 8 * c, PR[c])
        return PR

    def merge_faces(recv, table, w):
        first = w == 0
        n = 5 if first else 2
        plane = pl.ds(row(16, 0), NY)
        rows48 = pl.ds(row(0, 48), NZ, stride=PITCH)
        at = pl.ds(row(16, 48), 1)
        for c in range(2):
            K[2 * w + c, plane, :] = get(recv, table, "Z", (n - 2 + c) * NY, NY)
            K[2 * w + c, rows48, :] = get(recv, table, "Y", (n - 2 + c) * NZ, NZ)
            K[2 * w + c, at, :] = get(recv, table, "ZY", n - 2 + c, 1)
            if first:
                S[c, plane, :] = get(recv, table, "Z", c * NY, NY)
                S[c, rows48, :] = get(recv, table, "Y", c * NZ, NZ)
                S[c, at, :] = get(recv, table, "ZY", c, 1)
            S[c, pl.ds(row(-1, 0), NY), :] = get(recv, table, "z", c * NY, NY)
            S[c, pl.ds(row(0, -1), NZ, stride=PITCH), :] = get(recv, table, "y", c * NZ, NZ)
            S[c, pl.ds(row(16, -1), 1), :] = get(recv, table, "Zy", c, 1)
            S[c, pl.ds(row(-1, 48), 1), :] = get(recv, table, "zY", c, 1)
        if first:
            J[plane, :] = get(recv, table, "Z", 2 * NY, NY)
            J[rows48, :] = get(recv, table, "Y", 2 * NZ, NZ)
            J[at, :] = get(recv, table, "ZY", 2, 1)

    at_z = (zi == 17) & (tile < 6)
    at_y = (tile == 6) & (sub == 0) & (zi >= 1) & (zi <= 16)
    at_zy = (zi == 17) & (tile == 6) & (sub == 0)
    at_zm = (zi == 0) & (tile < 6)
    at_ym = (tile == 6) & (sub == 7) & (zi <= 15)
    at_zym = (lane == 118) & (sub == 7)
    at_yzm = (lane == 6) & (sub == 0)

    def upper(base, k, vz, vy, vzy, kzy=None):
        kzy = k if kzy is None else kzy
        base = jnp.where(at_z, roll(vz, 112 - 16 * k), base)
        base = jnp.where(at_y, roll(roll(vy, -k, 0), 6), base)
        return jnp.where(at_zy, roll(roll(vzy, -kzy, 0), 118), base)

    def lower(base, recv, table, c):
        base = jnp.where(at_zm, roll(get(recv, table, "Xz", 0), -112 + 16 * c), base)
        base = jnp.where(at_ym, roll(roll(get(recv, table, "Xy", 0), c, 0), -6), base)
        base = jnp.where(at_zym, roll(roll(get(recv, table, "XZy", 0), c, 0), 106), base)
        return jnp.where(at_yzm, roll(roll(get(recv, table, "XzY", 0), -c, 0), -106), base)

    def merge_columns(recv, table, w, PR, ES, EJ):
        first = w == 0
        n = 5 if first else 2

        def ext(k):
            base = get(recv, table, "X", 8 * k)
            return upper(base, k, *[get(recv, table, name, 0) for name in ("XZ", "XY", "XZY")])

        EK = [ext(n - 2 + c) for c in range(2)]
        if first:
            ES = [ext(c) for c in range(2)]
            EJ = ext(2)
        ES = [lower(ES[c], recv, table, c) for c in range(2)]
        HM = [
            upper(get(recv, table, "x", 8 * c), c, *[get(recv, table, name, 0) for name in ("xZ", "xY", "xZY")])
            for c in range(2)
        ]
        PM = [upper(PR[c], c, *[get(recv, table, name, 0) for name in ("PZ", "PY", "ZY")], kzy=5 + c) for c in range(2)]
        return EK, ES, EJ, HM, PM

    def shift_up(v):
        v = roll(v, 1, 0)
        return jnp.where(sub == 0, roll(v, 1), v)

    def shift_down(v):
        v = roll(v, -1, 0)
        return jnp.where(sub == 7, roll(v, -1), v)

    inside = (zi >= 1) & (zi <= 17) & ((tile < 6) | (sub == 0))

    def update_column(EK, ES, EJ, PM):
        for zp in range(2):
            for yp in range(2):
                member = inside & ((zi & 1) == 1 - zp) & ((sub & 1) == yp)
                local = []
                for c in range(2):
                    v = ES[c]
                    above = jnp.where(lane < 17 * TILES, roll(v, -7), 0.0)
                    near = shift_up(v) + shift_down(v) + roll(v, 7) + above + PM[c]
                    local.append(EJ * near + EK[c])
                scale = lax.rsqrt(1.0 + (local[0] * local[0] + local[1] * local[1]))
                ES = [jnp.where(member, local[c] * scale, ES[c]) for c in range(2)]
        return ES

    def spread(which, values):
        for c in range(2):
            v = values[c] if which == 0 else roll(values[c], -1)
            for q in range(TILES, 18 * TILES):
                XH[2 * which + c, pl.ds(8 * q, 8), :] = roll(v, -q)

    def update(w, base, n, stride, xp):
        def at(off):
            return pl.ds(base + off, n, stride=stride) if n > 1 else pl.ds(base + off, 1)

        lanes = lax.broadcasted_iota(jnp.int32, (n, 128), 1)
        member = (lanes & 1) == xp
        stiffness = J[at(0), :]
        local, centre = [], []
        for c in range(2):
            v = S[c, at(0), :]
            edge = XH[2 * xp + c, at(0), :]
            left, right = roll(v, 1), roll(v, -1)
            if xp == 0:
                left = jnp.where(lanes == 0, edge, left)
            else:
                right = jnp.where(lanes == 127, edge, right)
            near = (S[c, at(-1), :] + S[c, at(1), :]) + (S[c, at(-PITCH), :] + S[c, at(PITCH), :]) + (left + right)
            local.append(stiffness * near + K[2 * w + c, at(0), :])
            centre.append(v)
        q = local[0] * local[0] + local[1] * local[1]
        scale = lax.rsqrt(1.0 + q)
        for c in range(2):
            S[c, at(0), :] = jnp.where(member, local[c] * scale, centre[c])
        return q * scale

    def section(w, zp, yp, xp):
        energy = None
        for z in range(zp, NZ + 1 - zp, 2):
            e = update(w, row(z, yp), 24, 2, xp)
            if z < NZ:
                energy = e if energy is None else energy + e
        if yp == 0:
            update(w, row(zp, 48), 8, 2 * PITCH, xp)
            if zp == 0:
                update(w, row(16, 48), 1, 1, xp)
        energy = energy[0:8] + energy[8:16] + energy[16:24]
        t = 8 * w + 4 * zp + 2 * yp + xp
        EN[t] = jnp.where((lane & 1) == xp, energy, 0.0)

    build(send_a, TABLE_A, 0)
    PJ = pack_first(lambda r: J[pl.ds(r, 8), :])
    PK = [pack_first(lambda r, c=c: K[c, pl.ds(r, 8), :]) for c in range(2)]
    PR = build_columns(send_a, TABLE_A, 0, PJ, PK)
    pl.semaphore_wait(barrier, len(steps))
    for name in NAMES:
        copies_a[name].start()
    each(lambda z: load(z, 3).wait())
    PK = [pack_first(lambda r, c=c: K[2 + c, pl.ds(r, 8), :]) for c in range(2)]
    for name in COLUMNS:
        copies_a[name].wait_recv()
    EK, ES, EJ, HM, PM = merge_columns(recv_a, TABLE_A, 0, PR, None, None)
    spread(0, HM)
    ES = update_column(EK, ES, EJ, PM)
    spread(1, ES)
    for name in FACES:
        copies_a[name].wait_recv()
    merge_faces(recv_a, TABLE_A, 0)
    for t in range(8):
        section(0, t // 4, t // 2 % 2, t % 2)

    PR = build_columns(send_b, TABLE_B, 1, PJ, PK)
    build(send_b, TABLE_B, 1)
    for name in NAMES:
        copies_b[name].start()
    for name in NAMES:
        copies_a[name].wait_send()
    for name in FACES + tuple(COLUMNS):
        copies_b[name].wait_recv()
    merge_faces(recv_b, TABLE_B, 1)
    EK, ES, EJ, HM, PM = merge_columns(recv_b, TABLE_B, 1, PR, ES, EJ)
    spread(0, HM)
    section(1, 0, 0, 0)
    ES = update_column(EK, ES, EJ, PM)
    spread(1, ES)
    for t in range(1, 8):
        section(1, t // 4, t // 2 % 2, t % 2)

    sums = jnp.sum(jnp.sum(EN[...], axis=1), axis=1, keepdims=True)
    diagonal = lax.broadcasted_iota(jnp.int32, (16, 128), 0) == lax.broadcasted_iota(jnp.int32, (16, 128), 1)
    mine = jnp.sum(jnp.where(diagonal, jnp.broadcast_to(sums, (16, 128)), 0.0), axis=0, keepdims=True)
    index = (me[0] * ny + me[1]) * nx + me[2]
    erow[0] = mine
    ebuf[index] = mine

    coords = [[lax.rem(m + d, n) for d in range(n)] for m, n in zip(me, dims)]
    far = [[min(d, n - d) for d in range(n)] for n in dims]
    targets = [(a, b, c) for a in range(nz) for b in range(ny) for c in range(nx) if a + b + c]
    targets.sort(key=lambda t: -(far[0][t[0]] + far[1][t[1]] + (far[2][t[2]] + 1) // 2))
    for a, b, c in targets:
        pltpu.make_async_remote_copy(
            src_ref=erow.at[0],
            dst_ref=ebuf.at[index],
            send_sem=es_sem,
            recv_sem=er_sem,
            device_id=(coords[0][a], coords[1][b], coords[2][c]),
            device_id_type=MESH,
        ).start()
    for z in range(NZ):
        for c in range(2):
            out[c, z] = S[c, pl.ds(row(z, 0), NY), :]
    for name in NAMES:
        copies_b[name].wait_send()
    rest = pl.ds(0, total - 1)
    done = pltpu.make_async_remote_copy(
        src_ref=ebuf.at[rest],
        dst_ref=ebuf.at[rest],
        send_sem=es_sem,
        recv_sem=er_sem,
        device_id=me,
        device_id_type=MESH,
    )
    done.wait_recv()
    parts = [ebuf[i] for i in range(8)]
    for i in range(8, total):
        parts[i % 8] = parts[i % 8] + ebuf[i]
    while len(parts) > 1:
        parts = [a + b for a, b in zip(parts[::2], parts[1::2])]
    whole = parts[0]
    sites = float((NZ * nz) * (NY * ny) * (NX * nx) // 8)
    energy_out[...] = (-whole / sites)[0, :16]
    done.wait_send()


def body(dims, spins, kicks, stiffness):
    hbm = pl.BlockSpec(memory_space=pl.ANY)
    total = dims[0] * dims[1] * dims[2]
    vmem, dma = pltpu.VMEM, pltpu.SemaphoreType.DMA
    final, energy = pl.pallas_call(
        functools.partial(kernel, dims),
        out_shape=(
            jax.ShapeDtypeStruct((2, NZ, NY, NX), F32),
            jax.ShapeDtypeStruct((16,), F32),
        ),
        in_specs=[hbm] * 3,
        out_specs=(pl.BlockSpec(memory_space=vmem), pl.BlockSpec(memory_space=vmem)),
        scratch_shapes=[
            vmem((2, ROWS, 128), F32),
            vmem((ROWS, 128), F32),
            vmem((4, ROWS, 128), F32),
            vmem((4, ROWS, 128), F32),
            vmem((SIZE_A, 128), F32),
            vmem((SIZE_A, 128), F32),
            vmem((SIZE_B, 128), F32),
            vmem((SIZE_B, 128), F32),
            vmem((16, 8, 128), F32),
            vmem((total, 1, 128), F32),
            vmem((1, 1, 128), F32),
            dma((4, NZ)),
            dma((COUNT,)),
            dma((COUNT,)),
            dma((COUNT,)),
            dma((COUNT,)),
            dma,
            dma,
        ],
        compiler_params=pltpu.CompilerParams(collective_id=0, has_side_effects=True, vmem_limit_bytes=12 * 1024 * 1024),
    )(*[pltpu.with_memory_space_constraint(v, pltpu.HBM) for v in (spins, kicks, stiffness)])
    return final, energy


def solution(mesh):
    dims = tuple(mesh.shape[a] for a in ("gz", "gy", "gx"))
    return jax.shard_map(
        functools.partial(body, dims),
        mesh=mesh,
        in_specs=(P(None, "gz", "gy", "gx"), P(None, None, "gz", "gy", "gx"), P("gz", "gy", "gx")),
        out_specs=(P(None, "gz", "gy", "gx"), P()),
        check_vma=False,
    )
```

```python
import functools

import jax
import jax.numpy as jnp
from jax import lax
from jax.experimental import pallas as pl
from jax.experimental.pallas import tpu as pltpu
from jax.sharding import PartitionSpec as P

MESH = pl.DeviceIdType.MESH
F32 = jnp.float32
NZ, NY, NX = 16, 48, 128
PITCH = 56
ROWS = 19 * PITCH
TILES = 7

MESSAGES = {
    "XZY": ((-1, -1, -1), 8, 8),
    "XZy": ((-1, 1, -1), 8, 8),
    "XzY": ((1, -1, -1), 8, 8),
    "xZY": ((-1, -1, 1), 8, 8),
    "ZY": ((-1, -1, 0), 8, 8),
    "Zy": ((-1, 1, 0), 8, 8),
    "zY": ((1, -1, 0), 8, 8),
    "XZ": ((-1, 0, -1), 8, 8),
    "XY": ((0, -1, -1), 8, 8),
    "Xz": ((1, 0, -1), 8, 8),
    "Xy": ((0, 1, -1), 8, 8),
    "xZ": ((-1, 0, 1), 8, 8),
    "xY": ((0, -1, 1), 8, 8),
    "PZ": ((-1, 0, 0), 8, 8),
    "PY": ((0, -1, 0), 8, 8),
    "X": ((0, 0, -1), 40, 16),
    "x": ((0, 0, 1), 16, 16),
    "Z": ((-1, 0, 0), 240, 96),
    "z": ((1, 0, 0), 96, 96),
    "Y": ((0, -1, 0), 80, 32),
    "y": ((0, 1, 0), 32, 32),
}
NAMES = list(MESSAGES)
COUNT = len(NAMES)
FACES = ("Zy", "zY", "Z", "z", "Y", "y")
COLUMNS = [name for name in NAMES if name not in FACES]


def offsets(round_index):
    start, table = 0, {}
    for name in NAMES:
        size = MESSAGES[name][1 + round_index]
        table[name] = (start, size)
        start += size
    return table, start


TABLE_A, SIZE_A = offsets(0)
TABLE_B, SIZE_B = offsets(1)


def row(z, y):
    return (z + 1) * PITCH + y


def roll(v, shift, axis=1):
    shift = shift % v.shape[axis]
    return v if shift == 0 else pltpu.roll(v, shift, axis)


def kernel(dims, spins, kicks, stiff, out, energy_out, S, J, K, XH, fold, send_a, recv_a, send_b, recv_b, EN, ebuf, erow,
           load_sem, sa_sem, ra_sem, sb_sem, rb_sem, es_sem, er_sem):
    nz, ny, nx = dims
    total = nz * ny * nx
    me = (lax.axis_index("gz"), lax.axis_index("gy"), lax.axis_index("gx"))

    def device(step):
        return tuple(lax.rem(m + (d % n), n) for m, d, n in zip(me, step, dims))

    lane = lax.broadcasted_iota(jnp.int32, (8, 128), 1)
    sub = lax.broadcasted_iota(jnp.int32, (8, 128), 0)
    zi = (lane * 9363) >> 16
    tile = lane - zi * 7

    inner = (pl.ds(1, NZ), pl.ds(0, NY))
    planes = ROWS // PITCH
    loads = [
        pltpu.make_async_copy(spins, S.reshape(2, planes, PITCH, 128).at[(slice(None),) + inner], load_sem.at[0]),
        pltpu.make_async_copy(stiff, J.reshape(planes, PITCH, 128).at[inner], load_sem.at[1]),
    ]
    for w in range(2):
        whole = K.reshape(4, planes, PITCH, 128)
        loads.append(pltpu.make_async_copy(kicks.at[w], whole.at[(pl.ds(2 * w, 2),) + inner], load_sem.at[2 + w]))
    for copy in loads:
        copy.start()

    barrier = pltpu.get_barrier_semaphore()
    steps = sorted({MESSAGES[name][0] for name in NAMES})
    steps += [(0, 0, d) for d in range(2, nx - 1)]
    for s in steps:
        pl.semaphore_signal(barrier, inc=1, device_id=device(tuple(-d for d in s)), device_id_type=MESH)

    for copy in loads[:3]:
        copy.wait()

    zero_plane = jnp.zeros((PITCH, 128), F32)
    for c in range(2):
        S[c, pl.ds(18 * PITCH, PITCH), :] = zero_plane
        S[c, pl.ds(row(0, 49), NZ, stride=PITCH), :] = jnp.zeros((NZ, 128), F32)
        S[c, pl.ds(row(16, 49), 1), :] = jnp.zeros((1, 128), F32)

    lane3 = lane - ((lane * 21846) >> 16) * 3
    group = [((lane - r + 1) * 21846) >> 16 for r in range(3)]
    own_tiles = [(z + 1) * TILES + t for z in range(NZ) for t in range(6)]

    def pack_spins():
        cols = []
        for c in range(2):
            acc = [jnp.zeros((8, 128), F32) for _ in range(3)]
            for q in own_tiles:
                r = q % 3
                v = roll(S[c, pl.ds(8 * q, 8), :], q)
                acc[r] = jnp.where(group[r] == q // 3, v, acc[r])

            def pick(shift):
                a = [roll(v, shift) for v in acc]
                return jnp.where(lane3 == 0, a[0], jnp.where(lane3 == 1, a[1], a[2]))

            cols.append((pick(0), pick(-1), pick(1)))
        return [[cols[c][k] for c in range(2)] for k in range(3)]

    def pack_first(read):
        acc = jnp.zeros((8, 128), F32)
        for q in own_tiles:
            acc = jnp.where(lane == q, roll(read(8 * q), q), acc)
        return acc

    def zplus(v):
        return roll(v, -7)

    def yplus(v):
        return roll(v, -1, 0)

    def copies(send, recv, table, ssem, rsem):
        result = {}
        for i, name in enumerate(NAMES):
            start, size = table[name]
            part = pl.ds(start, size)
            result[name] = pltpu.make_async_remote_copy(
                src_ref=send.at[part, :],
                dst_ref=recv.at[part, :],
                send_sem=ssem.at[i],
                recv_sem=rsem.at[i],
                device_id=device(MESSAGES[name][0]),
                device_id_type=MESH,
            )
        return result

    def put(send, table, name, at, value):
        send[pl.ds(table[name][0] + at, value.shape[0]), :] = value

    def get(recv, table, name, at, size=8):
        return recv[pl.ds(table[name][0] + at, size), :]

    copies_a = copies(send_a, recv_a, TABLE_A, sa_sem, ra_sem)
    copies_b = copies(send_b, recv_b, TABLE_B, sb_sem, rb_sem)

    def build(send, table, w):
        first = w == 0
        n = 5 if first else 2
        J0 = J[pl.ds(row(0, 0), NY), :]
        for c in range(2):
            kc = K[2 * w + c, pl.ds(row(0, 0), NY), :] + J0 * S[c, pl.ds(row(1, 0), NY), :]
            put(send, table, "Z", (n - 2 + c) * NY, kc)
            if first:
                put(send, table, "Z", c * NY, S[c, pl.ds(row(0, 0), NY), :])
            put(send, table, "z", c * NY, S[c, pl.ds(row(15, 0), NY), :])
        if first:
            put(send, table, "Z", 2 * NY, J0)
        rows0 = pl.ds(row(0, 0), NZ, stride=PITCH)
        rows1 = pl.ds(row(0, 1), NZ, stride=PITCH)
        rows47 = pl.ds(row(0, 47), NZ, stride=PITCH)
        Jy = J[rows0, :]
        for c in range(2):
            kc = K[2 * w + c, rows0, :] + Jy * S[c, rows1, :]
            put(send, table, "Y", (n - 2 + c) * NZ, kc)
            if first:
                put(send, table, "Y", c * NZ, S[c, rows0, :])
            put(send, table, "y", c * NZ, S[c, rows47, :])
        if first:
            put(send, table, "Y", 2 * NZ, Jy)
        at = pl.ds(row(0, 0), 1)
        for c in range(2):
            kc = K[2 * w + c, at, :] + J[at, :] * (S[c, pl.ds(row(1, 0), 1), :] + S[c, pl.ds(row(0, 1), 1), :])
            put(send, table, "ZY", n - 2 + c, kc)
            if first:
                put(send, table, "ZY", c, S[c, at, :])
            put(send, table, "Zy", c, S[c, pl.ds(row(0, 47), 1), :])
            put(send, table, "zY", c, S[c, pl.ds(row(15, 0), 1), :])
        if first:
            put(send, table, "ZY", 2, J[at, :])

    def by_lanes(values, shift=0):
        acc = values[0]
        for k in range(1, len(values)):
            acc = jnp.where((lane >> 4) == k, roll(values[k], 16 * k), acc)
        return acc

    def by_rows(values):
        acc = values[0]
        for k in range(1, len(values)):
            acc = jnp.where(sub == k, roll(values[k], k, 0), acc)
        return acc

    def build_columns(send, table, w, PJ, PK):
        first = w == 0
        PS, PT, PR = pack_spins()
        parts = {name: [] for name in ("X", "XZ", "XY", "XZY")}
        for c in range(2):
            zs, ys = zplus(PS[c]), yplus(PS[c])
            sums = {"X": PT[c], "XZ": PT[c] + zs, "XY": PT[c] + ys, "XZY": PT[c] + zs + ys}
            for name, value in sums.items():
                parts[name].append(PK[c] + PJ * value)
        if first:
            parts = {name: PS + [PJ] + value for name, value in parts.items()}
        put(send, table, "XZY", 0, by_rows(parts["XZY"]))
        put(send, table, "XZ", 0, by_lanes(parts["XZ"]))
        put(send, table, "XY", 0, by_rows(parts["XY"]))
        for k, value in enumerate(parts["X"]):
            put(send, table, "X", 8 * k, value)
        last = jnp.where(sub == 6, roll(PS[1], -1, 0), PS[0])
        put(send, table, "XZy", 0, last)
        put(send, table, "Xy", 0, last)
        put(send, table, "XzY", 0, by_rows(PS))
        put(send, table, "Xz", 0, jnp.where((lane >> 4) == 6, roll(PS[1], -16), PS[0]))
        rows, lanes = by_rows(PR), by_lanes(PR)
        for name in ("xZY", "xY", "PY"):
            put(send, table, name, 0, rows)
        for name in ("xZ", "PZ"):
            put(send, table, name, 0, lanes)
        put(send, table, "ZY", 5, rows[0:2])
        for c in range(2):
            put(send, table, "x", 8 * c, PR[c])
        return PR

    def merge_faces(recv, table, w):
        first = w == 0
        n = 5 if first else 2
        plane = pl.ds(row(16, 0), NY)
        rows48 = pl.ds(row(0, 48), NZ, stride=PITCH)
        at = pl.ds(row(16, 48), 1)
        for c in range(2):
            K[2 * w + c, plane, :] = get(recv, table, "Z", (n - 2 + c) * NY, NY)
            K[2 * w + c, rows48, :] = get(recv, table, "Y", (n - 2 + c) * NZ, NZ)
            K[2 * w + c, at, :] = get(recv, table, "ZY", n - 2 + c, 1)
            if first:
                S[c, plane, :] = get(recv, table, "Z", c * NY, NY)
                S[c, rows48, :] = get(recv, table, "Y", c * NZ, NZ)
                S[c, at, :] = get(recv, table, "ZY", c, 1)
            S[c, pl.ds(row(-1, 0), NY), :] = get(recv, table, "z", c * NY, NY)
            S[c, pl.ds(row(0, -1), NZ, stride=PITCH), :] = get(recv, table, "y", c * NZ, NZ)
            S[c, pl.ds(row(16, -1), 1), :] = get(recv, table, "Zy", c, 1)
            S[c, pl.ds(row(-1, 48), 1), :] = get(recv, table, "zY", c, 1)
        if first:
            J[plane, :] = get(recv, table, "Z", 2 * NY, NY)
            J[rows48, :] = get(recv, table, "Y", 2 * NZ, NZ)
            J[at, :] = get(recv, table, "ZY", 2, 1)

    at_z = (zi == 17) & (tile < 6)
    at_y = (tile == 6) & (sub == 0) & (zi >= 1) & (zi <= 16)
    at_zy = (zi == 17) & (tile == 6) & (sub == 0)
    at_zm = (zi == 0) & (tile < 6)
    at_ym = (tile == 6) & (sub == 7) & (zi <= 15)
    at_zym = (lane == 118) & (sub == 7)
    at_yzm = (lane == 6) & (sub == 0)

    def upper(base, k, vz, vy, vzy, kzy=None):
        kzy = k if kzy is None else kzy
        base = jnp.where(at_z, roll(vz, 112 - 16 * k), base)
        base = jnp.where(at_y, roll(roll(vy, -k, 0), 6), base)
        return jnp.where(at_zy, roll(roll(vzy, -kzy, 0), 118), base)

    def lower(base, recv, table, c):
        base = jnp.where(at_zm, roll(get(recv, table, "Xz", 0), -112 + 16 * c), base)
        base = jnp.where(at_ym, roll(roll(get(recv, table, "Xy", 0), c, 0), -6), base)
        base = jnp.where(at_zym, roll(roll(get(recv, table, "XZy", 0), c, 0), 106), base)
        return jnp.where(at_yzm, roll(roll(get(recv, table, "XzY", 0), -c, 0), -106), base)

    def merge_columns(recv, table, w, PR, ES, EJ):
        first = w == 0
        n = 5 if first else 2

        def ext(k):
            base = get(recv, table, "X", 8 * k)
            return upper(base, k, *[get(recv, table, name, 0) for name in ("XZ", "XY", "XZY")])

        EK = [ext(n - 2 + c) for c in range(2)]
        if first:
            ES = [ext(c) for c in range(2)]
            EJ = ext(2)
        ES = [lower(ES[c], recv, table, c) for c in range(2)]
        HM = [
            upper(get(recv, table, "x", 8 * c), c, *[get(recv, table, name, 0) for name in ("xZ", "xY", "xZY")])
            for c in range(2)
        ]
        PM = [upper(PR[c], c, *[get(recv, table, name, 0) for name in ("PZ", "PY", "ZY")], kzy=5 + c) for c in range(2)]
        return EK, ES, EJ, HM, PM

    def shift_up(v):
        v = roll(v, 1, 0)
        return jnp.where(sub == 0, roll(v, 1), v)

    def shift_down(v):
        v = roll(v, -1, 0)
        return jnp.where(sub == 7, roll(v, -1), v)

    inside = (zi >= 1) & (zi <= 17) & ((tile < 6) | (sub == 0))

    def update_column(EK, ES, EJ, PM):
        for zp in range(2):
            for yp in range(2):
                member = inside & ((zi & 1) == 1 - zp) & ((sub & 1) == yp)
                local = []
                for c in range(2):
                    v = ES[c]
                    above = jnp.where(lane < 17 * TILES, roll(v, -7), 0.0)
                    near = shift_up(v) + shift_down(v) + roll(v, 7) + above + PM[c]
                    local.append(EJ * near + EK[c])
                scale = lax.rsqrt(1.0 + (local[0] * local[0] + local[1] * local[1]))
                ES = [jnp.where(member, local[c] * scale, ES[c]) for c in range(2)]
        return ES

    def spread(which, values):
        result = []
        for c in range(2):
            v = values[c]
            fold[2 * which + c, 0:8] = v
            fold[2 * which + c, 8:16] = roll(v, -1)
            result.append([fold[2 * which + c, pl.ds(yp, 8, stride=2)] for yp in range(2)])
            for z in range(NZ + 1):
                XH[2 * which + c, pl.ds(z, 1), :] = roll(v, 127 * which - ((z + 1) * TILES + 6))[0:1]
        return result

    def update(w, base, n, stride, xp, edges):
        def at(off):
            return pl.ds(base + off, n, stride=stride) if n > 1 else pl.ds(base + off, 1)

        lanes = lax.broadcasted_iota(jnp.int32, (n, 128), 1)
        member = (lanes & 1) == xp
        stiffness = J[at(0), :]
        local, centre = [], []
        for c in range(2):
            v = S[c, at(0), :]
            edge = edges[c]
            left, right = roll(v, 1), roll(v, -1)
            if xp == 0:
                left = jnp.where(lanes == 0, edge, left)
            else:
                right = jnp.where(lanes == 127, edge, right)
            near = (S[c, at(-1), :] + S[c, at(1), :]) + (S[c, at(-PITCH), :] + S[c, at(PITCH), :]) + (left + right)
            local.append(stiffness * near + K[2 * w + c, at(0), :])
            centre.append(v)
        q = local[0] * local[0] + local[1] * local[1]
        scale = lax.rsqrt(1.0 + q)
        for c in range(2):
            S[c, at(0), :] = jnp.where(member, local[c] * scale, centre[c])
        return q * scale

    def section(w, zp, yp, xp, columns):
        energy = None
        for z in range(zp, NZ + 1 - zp, 2):
            first = 127 * xp - (z + 1) * TILES
            edges = [
                jnp.concatenate([roll(columns[c][yp], first - 2 * j) for j in range(3)], axis=0) for c in range(2)
            ]
            e = update(w, row(z, yp), 24, 2, xp, edges)
            if z < NZ:
                energy = e if energy is None else energy + e
        if yp == 0:
            edges = [XH[2 * xp + c, pl.ds(zp, 8, stride=2), :] for c in range(2)]
            update(w, row(zp, 48), 8, 2 * PITCH, xp, edges)
            if zp == 0:
                update(w, row(16, 48), 1, 1, xp, [XH[2 * xp + c, pl.ds(NZ, 1), :] for c in range(2)])
        energy = energy[0:8] + energy[8:16] + energy[16:24]
        t = 8 * w + 4 * zp + 2 * yp + xp
        EN[t] = jnp.where((lane & 1) == xp, energy, 0.0)

    build(send_a, TABLE_A, 0)
    PJ = pack_first(lambda r: J[pl.ds(r, 8), :])
    PK = [pack_first(lambda r, c=c: K[c, pl.ds(r, 8), :]) for c in range(2)]
    PR = build_columns(send_a, TABLE_A, 0, PJ, PK)
    pl.semaphore_wait(barrier, len(steps))
    for name in NAMES:
        copies_a[name].start()
    loads[3].wait()
    PK = [pack_first(lambda r, c=c: K[2 + c, pl.ds(r, 8), :]) for c in range(2)]
    for name in COLUMNS:
        copies_a[name].wait_recv()
    EK, ES, EJ, HM, PM = merge_columns(recv_a, TABLE_A, 0, PR, None, None)
    columns = [spread(0, HM)]
    ES = update_column(EK, ES, EJ, PM)
    columns.append(spread(1, ES))
    for name in FACES:
        copies_a[name].wait_recv()
    merge_faces(recv_a, TABLE_A, 0)
    for t in range(8):
        section(0, t // 4, t // 2 % 2, t % 2, columns[t % 2])

    PR = build_columns(send_b, TABLE_B, 1, PJ, PK)
    build(send_b, TABLE_B, 1)
    for name in NAMES:
        copies_b[name].start()
    for name in NAMES:
        copies_a[name].wait_send()
    for name in FACES + tuple(COLUMNS):
        copies_b[name].wait_recv()
    merge_faces(recv_b, TABLE_B, 1)
    EK, ES, EJ, HM, PM = merge_columns(recv_b, TABLE_B, 1, PR, ES, EJ)
    columns = [spread(0, HM)]
    section(1, 0, 0, 0, columns[0])
    ES = update_column(EK, ES, EJ, PM)
    columns.append(spread(1, ES))
    for t in range(1, 8):
        section(1, t // 4, t // 2 % 2, t % 2, columns[t % 2])

    sums = jnp.sum(jnp.sum(EN[...], axis=1), axis=1, keepdims=True)
    diagonal = lax.broadcasted_iota(jnp.int32, (16, 128), 0) == lax.broadcasted_iota(jnp.int32, (16, 128), 1)
    mine = jnp.sum(jnp.where(diagonal, jnp.broadcast_to(sums, (16, 128)), 0.0), axis=0, keepdims=True)
    index = (me[0] * ny + me[1]) * nx + me[2]
    erow[0] = mine
    ebuf[index] = mine

    coords = [[lax.rem(m + d, n) for d in range(n)] for m, n in zip(me, dims)]
    far = [[min(d, n - d) for d in range(n)] for n in dims]
    targets = [(a, b, c) for a in range(nz) for b in range(ny) for c in range(nx) if a + b + c]
    targets.sort(key=lambda t: -(far[0][t[0]] + far[1][t[1]] + (far[2][t[2]] + 1) // 2))
    for a, b, c in targets:
        pltpu.make_async_remote_copy(
            src_ref=erow.at[0],
            dst_ref=ebuf.at[index],
            send_sem=es_sem,
            recv_sem=er_sem,
            device_id=(coords[0][a], coords[1][b], coords[2][c]),
            device_id_type=MESH,
        ).start()
    for z in range(NZ):
        for c in range(2):
            out[c, z] = S[c, pl.ds(row(z, 0), NY), :]
    for name in NAMES:
        copies_b[name].wait_send()
    rest = pl.ds(0, total - 1)
    done = pltpu.make_async_remote_copy(
        src_ref=ebuf.at[rest],
        dst_ref=ebuf.at[rest],
        send_sem=es_sem,
        recv_sem=er_sem,
        device_id=me,
        device_id_type=MESH,
    )
    done.wait_recv()
    parts = [ebuf[i] for i in range(8)]
    for i in range(8, total):
        parts[i % 8] = parts[i % 8] + ebuf[i]
    while len(parts) > 1:
        parts = [a + b for a, b in zip(parts[::2], parts[1::2])]
    whole = parts[0]
    sites = float((NZ * nz) * (NY * ny) * (NX * nx) // 8)
    energy_out[...] = (-whole / sites)[0, :16]
    done.wait_send()


def body(dims, spins, kicks, stiffness):
    hbm = pl.BlockSpec(memory_space=pl.ANY)
    total = dims[0] * dims[1] * dims[2]
    vmem, dma = pltpu.VMEM, pltpu.SemaphoreType.DMA
    final, energy = pl.pallas_call(
        functools.partial(kernel, dims),
        out_shape=(
            jax.ShapeDtypeStruct((2, NZ, NY, NX), F32),
            jax.ShapeDtypeStruct((16,), F32),
        ),
        in_specs=[hbm] * 3,
        out_specs=(pl.BlockSpec(memory_space=vmem), pl.BlockSpec(memory_space=vmem)),
        scratch_shapes=[
            vmem((2, ROWS, 128), F32),
            vmem((ROWS, 128), F32),
            vmem((4, ROWS, 128), F32),
            vmem((4, 24, 128), F32),
            vmem((4, 16, 128), F32),
            vmem((SIZE_A, 128), F32),
            vmem((SIZE_A, 128), F32),
            vmem((SIZE_B, 128), F32),
            vmem((SIZE_B, 128), F32),
            vmem((16, 8, 128), F32),
            vmem((total, 1, 128), F32),
            vmem((1, 1, 128), F32),
            dma((4,)),
            dma((COUNT,)),
            dma((COUNT,)),
            dma((COUNT,)),
            dma((COUNT,)),
            dma,
            dma,
        ],
        compiler_params=pltpu.CompilerParams(collective_id=0, has_side_effects=True, vmem_limit_bytes=12 * 1024 * 1024),
    )(*[pltpu.with_memory_space_constraint(v, pltpu.HBM) for v in (spins, kicks, stiffness)])
    def finish(final, energy, out, energy_out, sem):
        copies = [pltpu.make_async_copy(final, out, sem.at[0]), pltpu.make_async_copy(energy, energy_out, sem.at[1])]
        for copy in copies:
            copy.start()
        for copy in copies:
            copy.wait()

    final, energy = [pltpu.with_memory_space_constraint(v, pltpu.VMEM) for v in (final, energy)]
    return pl.pallas_call(
        finish,
        out_shape=(jax.ShapeDtypeStruct((2, NZ, NY, NX), F32), jax.ShapeDtypeStruct((16,), F32)),
        in_specs=[hbm, hbm],
        out_specs=(hbm, hbm),
        scratch_shapes=[dma((2,))],
        compiler_params=pltpu.CompilerParams(vmem_limit_bytes=1024 * 1024),
    )(final, energy)


def solution(mesh):
    dims = tuple(mesh.shape[a] for a in ("gz", "gy", "gx"))
    return jax.shard_map(
        functools.partial(body, dims),
        mesh=mesh,
        in_specs=(P(None, "gz", "gy", "gx"), P(None, None, "gz", "gy", "gx"), P("gz", "gy", "gx")),
        out_specs=(P(None, "gz", "gy", "gx"), P()),
        check_vma=False,
    )
```

```python
import functools

import jax
import jax.numpy as jnp
from jax import lax
from jax.experimental import pallas as pl
from jax.experimental.pallas import tpu as pltpu
from jax.sharding import PartitionSpec as P

MESH = pl.DeviceIdType.MESH
F32 = jnp.float32
NZ, NY, NX = 16, 48, 128
PITCH = 56
ROWS = 19 * PITCH
TILES = 7

MESSAGES = {
    "XZY": ((-1, -1, -1), 8, 8),
    "XZy": ((-1, 1, -1), 8, 8),
    "XzY": ((1, -1, -1), 8, 8),
    "xZY": ((-1, -1, 1), 8, 8),
    "ZY": ((-1, -1, 0), 8, 8),
    "Zy": ((-1, 1, 0), 8, 8),
    "zY": ((1, -1, 0), 8, 8),
    "XZ": ((-1, 0, -1), 8, 8),
    "XY": ((0, -1, -1), 8, 8),
    "Xz": ((1, 0, -1), 8, 8),
    "Xy": ((0, 1, -1), 8, 8),
    "xZ": ((-1, 0, 1), 8, 8),
    "xY": ((0, -1, 1), 8, 8),
    "PZ": ((-1, 0, 0), 8, 8),
    "PY": ((0, -1, 0), 8, 8),
    "X": ((0, 0, -1), 40, 16),
    "x": ((0, 0, 1), 16, 16),
    "z": ((1, 0, 0), 96, 96),
    "Y": ((0, -1, 0), 80, 32),
    "y": ((0, 1, 0), 32, 32),
    "Z": ((-1, 0, 0), 96, 96),
    "ZS": ((-1, 0, 0), 144, 0),
}
NAMES = list(MESSAGES)
COUNT = len(NAMES)
TOP = ("Z", "ZS")
FACES = ("Zy", "zY", "z", "Y", "y")
LEFT = ("x", "xZ", "xY", "ZY")
RIGHT = [name for name in NAMES if name not in FACES + TOP + LEFT + ("xZY",)]
NAMES_B = [name for name in NAMES if name != "ZS"]


def away(name):
    return sum(abs(d) for d in MESSAGES[name][0])


def offsets(round_index):
    start, table = 0, {}
    for name in NAMES:
        size = MESSAGES[name][1 + round_index]
        table[name] = (start, size)
        start += size
    return table, start


TABLE_A, SIZE_A = offsets(0)
TABLE_B, SIZE_B = offsets(1)


def row(z, y):
    return (z + 1) * PITCH + y


def roll(v, shift, axis=1):
    shift = shift % v.shape[axis]
    return v if shift == 0 else pltpu.roll(v, shift, axis)


def kernel(dims, spins, kicks, stiff, out, energy_out, S, J, K, XH, fold, send_a, recv_a, send_b, recv_b, EN, ebuf, erow,
           load_sem, token, sa_sem, ra_sem, sb_sem, rb_sem, es_sem, er_sem):
    nz, ny, nx = dims
    total = nz * ny * nx
    me = (lax.axis_index("gz"), lax.axis_index("gy"), lax.axis_index("gx"))

    def device(step):
        return tuple(lax.rem(m + (d % n), n) for m, d, n in zip(me, step, dims))

    lane = lax.broadcasted_iota(jnp.int32, (8, 128), 1)
    sub = lax.broadcasted_iota(jnp.int32, (8, 128), 0)
    zi = (lane * 9363) >> 16
    tile = lane - zi * 7

    inner = (pl.ds(1, NZ), pl.ds(0, NY))
    planes = ROWS // PITCH
    loads = [
        pltpu.make_async_copy(spins, S.reshape(2, planes, PITCH, 128).at[(slice(None),) + inner], load_sem.at[0]),
        pltpu.make_async_copy(stiff, J.reshape(planes, PITCH, 128).at[inner], load_sem.at[1]),
    ]
    for w in range(2):
        whole = K.reshape(4, planes, PITCH, 128)
        loads.append(pltpu.make_async_copy(kicks.at[w], whole.at[(pl.ds(2 * w, 2),) + inner], load_sem.at[2 + w]))
    for copy in loads:
        copy.start()

    barrier = pltpu.get_barrier_semaphore()
    steps = sorted({MESSAGES[name][0] for name in NAMES if away(name) < 3})
    steps += [(0, 0, d) for d in range(2, nx - 1)]
    steps.sort(key=lambda step: -sum(map(abs, step)))
    for s in steps:
        pl.semaphore_signal(barrier, inc=1, device_id=device(tuple(-d for d in s)), device_id_type=MESH)

    for copy in loads[:3]:
        copy.wait()

    zero_plane = jnp.zeros((PITCH, 128), F32)
    for c in range(2):
        S[c, pl.ds(18 * PITCH, PITCH), :] = zero_plane
        S[c, pl.ds(row(0, 49), NZ, stride=PITCH), :] = jnp.zeros((NZ, 128), F32)
        S[c, pl.ds(row(16, 49), 1), :] = jnp.zeros((1, 128), F32)

    lane3 = lane - ((lane * 21846) >> 16) * 3
    group = [((lane - r + 1) * 21846) >> 16 for r in range(3)]
    own_tiles = [(z + 1) * TILES + t for z in range(NZ) for t in range(6)]

    def pack_spins():
        cols = []
        for c in range(2):
            acc = [jnp.zeros((8, 128), F32) for _ in range(3)]
            for q in own_tiles:
                r = q % 3
                v = roll(S[c, pl.ds(8 * q, 8), :], q)
                acc[r] = jnp.where(group[r] == q // 3, v, acc[r])

            def pick(shift):
                a = [roll(v, shift) for v in acc]
                return jnp.where(lane3 == 0, a[0], jnp.where(lane3 == 1, a[1], a[2]))

            cols.append((pick(0), pick(-1), pick(1)))
        return [[cols[c][k] for c in range(2)] for k in range(3)]

    def pack_first(read):
        acc = jnp.zeros((8, 128), F32)
        for q in own_tiles:
            acc = jnp.where(lane == q, roll(read(8 * q), q), acc)
        return acc

    def zplus(v):
        return roll(v, -7)

    def yplus(v):
        return roll(v, -1, 0)

    def copies(send, recv, table, ssem, rsem):
        result = {}
        for i, name in enumerate(NAMES):
            start, size = table[name]
            if size == 0:
                continue
            part = pl.ds(start, size)
            result[name] = pltpu.make_async_remote_copy(
                src_ref=send.at[part, :],
                dst_ref=recv.at[part, :],
                send_sem=ssem.at[i],
                recv_sem=rsem.at[i],
                device_id=device(MESSAGES[name][0]),
                device_id_type=MESH,
            )
        return result

    def put(send, table, name, at, value):
        send[pl.ds(table[name][0] + at, value.shape[0]), :] = value

    def get(recv, table, name, at, size=8):
        return recv[pl.ds(table[name][0] + at, size), :]

    copies_a = copies(send_a, recv_a, TABLE_A, sa_sem, ra_sem)
    copies_b = copies(send_b, recv_b, TABLE_B, sb_sem, rb_sem)

    def build(send, table, w):
        first = w == 0
        n = 5 if first else 2
        J0 = J[pl.ds(row(0, 0), NY), :]
        for c in range(2):
            kc = K[2 * w + c, pl.ds(row(0, 0), NY), :] + J0 * S[c, pl.ds(row(1, 0), NY), :]
            put(send, table, "Z", c * NY, kc)
            if first:
                put(send, table, "ZS", c * NY, S[c, pl.ds(row(0, 0), NY), :])
            put(send, table, "z", c * NY, S[c, pl.ds(row(15, 0), NY), :])
        if first:
            put(send, table, "ZS", 2 * NY, J0)
        rows0 = pl.ds(row(0, 0), NZ, stride=PITCH)
        rows1 = pl.ds(row(0, 1), NZ, stride=PITCH)
        rows47 = pl.ds(row(0, 47), NZ, stride=PITCH)
        Jy = J[rows0, :]
        for c in range(2):
            kc = K[2 * w + c, rows0, :] + Jy * S[c, rows1, :]
            put(send, table, "Y", (n - 2 + c) * NZ, kc)
            if first:
                put(send, table, "Y", c * NZ, S[c, rows0, :])
            put(send, table, "y", c * NZ, S[c, rows47, :])
        if first:
            put(send, table, "Y", 2 * NZ, Jy)
        at = pl.ds(row(0, 0), 1)
        for c in range(2):
            kc = K[2 * w + c, at, :] + J[at, :] * (S[c, pl.ds(row(1, 0), 1), :] + S[c, pl.ds(row(0, 1), 1), :])
            put(send, table, "ZY", n - 2 + c, kc)
            if first:
                put(send, table, "ZY", c, S[c, at, :])
            put(send, table, "Zy", c, S[c, pl.ds(row(0, 47), 1), :])
            put(send, table, "zY", c, S[c, pl.ds(row(15, 0), 1), :])
        if first:
            put(send, table, "ZY", 2, J[at, :])

    def by_lanes(values, shift=0):
        acc = values[0]
        for k in range(1, len(values)):
            acc = jnp.where((lane >> 4) == k, roll(values[k], 16 * k), acc)
        return acc

    def by_rows(values):
        acc = values[0]
        for k in range(1, len(values)):
            acc = jnp.where(sub == k, roll(values[k], k, 0), acc)
        return acc

    def build_columns(send, table, w, PJ, PK):
        first = w == 0
        PS, PT, PR = pack_spins()
        parts = {name: [] for name in ("X", "XZ", "XY", "XZY")}
        for c in range(2):
            zs, ys = zplus(PS[c]), yplus(PS[c])
            sums = {"X": PT[c], "XZ": PT[c] + zs, "XY": PT[c] + ys, "XZY": PT[c] + zs + ys}
            for name, value in sums.items():
                parts[name].append(PK[c] + PJ * value)
        if first:
            parts = {name: PS + [PJ] + value for name, value in parts.items()}
        put(send, table, "XZY", 0, by_rows(parts["XZY"]))
        put(send, table, "XZ", 0, by_lanes(parts["XZ"]))
        put(send, table, "XY", 0, by_rows(parts["XY"]))
        for k, value in enumerate(parts["X"]):
            put(send, table, "X", 8 * k, value)
        last = jnp.where(sub == 6, roll(PS[1], -1, 0), PS[0])
        put(send, table, "XZy", 0, last)
        put(send, table, "Xy", 0, last)
        put(send, table, "XzY", 0, by_rows(PS))
        put(send, table, "Xz", 0, jnp.where((lane >> 4) == 6, roll(PS[1], -16), PS[0]))
        rows, lanes = by_rows(PR), by_lanes(PR)
        for name in ("xZY", "xY", "PY"):
            put(send, table, name, 0, rows)
        for name in ("xZ", "PZ"):
            put(send, table, name, 0, lanes)
        put(send, table, "ZY", 5, rows[0:2])
        for c in range(2):
            put(send, table, "x", 8 * c, PR[c])
        return PR

    def merge_faces(recv, table, w):
        first = w == 0
        n = 5 if first else 2
        rows48 = pl.ds(row(0, 48), NZ, stride=PITCH)
        at = pl.ds(row(16, 48), 1)
        for c in range(2):
            K[2 * w + c, rows48, :] = get(recv, table, "Y", (n - 2 + c) * NZ, NZ)
            K[2 * w + c, at, :] = get(recv, table, "ZY", n - 2 + c, 1)
            if first:
                S[c, rows48, :] = get(recv, table, "Y", c * NZ, NZ)
                S[c, at, :] = get(recv, table, "ZY", c, 1)
            S[c, pl.ds(row(-1, 0), NY), :] = get(recv, table, "z", c * NY, NY)
            S[c, pl.ds(row(0, -1), NZ, stride=PITCH), :] = get(recv, table, "y", c * NZ, NZ)
            S[c, pl.ds(row(16, -1), 1), :] = get(recv, table, "Zy", c, 1)
            S[c, pl.ds(row(-1, 48), 1), :] = get(recv, table, "zY", c, 1)
        if first:
            J[rows48, :] = get(recv, table, "Y", 2 * NZ, NZ)
            J[at, :] = get(recv, table, "ZY", 2, 1)

    def merge_top(recv, table, w):
        plane = pl.ds(row(16, 0), NY)
        for c in range(2):
            K[2 * w + c, plane, :] = get(recv, table, "Z", c * NY, NY)
            if w == 0:
                S[c, plane, :] = get(recv, table, "ZS", c * NY, NY)
        if w == 0:
            J[plane, :] = get(recv, table, "ZS", 2 * NY, NY)

    at_z = (zi == 17) & (tile < 6)
    at_y = (tile == 6) & (sub == 0) & (zi >= 1) & (zi <= 16)
    at_zy = (zi == 17) & (tile == 6) & (sub == 0)
    at_zm = (zi == 0) & (tile < 6)
    at_ym = (tile == 6) & (sub == 7) & (zi <= 15)
    at_zym = (lane == 118) & (sub == 7)
    at_yzm = (lane == 6) & (sub == 0)

    def upper(base, k, vz, vy, vzy, kzy=None):
        kzy = k if kzy is None else kzy
        base = jnp.where(at_z, roll(vz, 112 - 16 * k), base)
        base = jnp.where(at_y, roll(roll(vy, -k, 0), 6), base)
        return jnp.where(at_zy, roll(roll(vzy, -kzy, 0), 118), base)

    def lower(base, recv, table, c):
        base = jnp.where(at_zm, roll(get(recv, table, "Xz", 0), -112 + 16 * c), base)
        base = jnp.where(at_ym, roll(roll(get(recv, table, "Xy", 0), c, 0), -6), base)
        base = jnp.where(at_zym, roll(roll(get(recv, table, "XZy", 0), c, 0), 106), base)
        return jnp.where(at_yzm, roll(roll(get(recv, table, "XzY", 0), -c, 0), -106), base)

    def merge_left(recv, table):
        result = []
        for c in range(2):
            base = get(recv, table, "x", 8 * c)
            base = jnp.where(at_z, roll(get(recv, table, "xZ", 0), 112 - 16 * c), base)
            result.append(jnp.where(at_y, roll(roll(get(recv, table, "xY", 0), -c, 0), 6), base))
        return result

    def merge_columns(recv, table, w, PR, ES, EJ):
        first = w == 0
        n = 5 if first else 2

        def ext(k):
            base = get(recv, table, "X", 8 * k)
            return upper(base, k, *[get(recv, table, name, 0) for name in ("XZ", "XY", "XZY")])

        EK = [ext(n - 2 + c) for c in range(2)]
        if first:
            ES = [ext(c) for c in range(2)]
            EJ = ext(2)
        ES = [lower(ES[c], recv, table, c) for c in range(2)]
        PM = [upper(PR[c], c, *[get(recv, table, name, 0) for name in ("PZ", "PY", "ZY")], kzy=5 + c) for c in range(2)]
        return EK, ES, EJ, PM

    def shift_up(v):
        v = roll(v, 1, 0)
        return jnp.where(sub == 0, roll(v, 1), v)

    def shift_down(v):
        v = roll(v, -1, 0)
        return jnp.where(sub == 7, roll(v, -1), v)

    inside = (zi >= 1) & (zi <= 17) & ((tile < 6) | (sub == 0))

    def update_column(EK, ES, EJ, PM):
        for zp in range(2):
            for yp in range(2):
                member = inside & ((zi & 1) == 1 - zp) & ((sub & 1) == yp)
                local = []
                for c in range(2):
                    v = ES[c]
                    above = jnp.where(lane < 17 * TILES, roll(v, -7), 0.0)
                    near = shift_up(v) + shift_down(v) + roll(v, 7) + above + PM[c]
                    local.append(EJ * near + EK[c])
                scale = lax.rsqrt(1.0 + (local[0] * local[0] + local[1] * local[1]))
                ES = [jnp.where(member, local[c] * scale, ES[c]) for c in range(2)]
        return ES

    def spread(which, values):
        result = []
        for c in range(2):
            v = values[c]
            fold[2 * which + c, 0:8] = v
            fold[2 * which + c, 8:16] = roll(v, -1)
            result.append([fold[2 * which + c, pl.ds(yp, 8, stride=2)] for yp in range(2)])
            for z in range(NZ + which):
                XH[2 * which + c, pl.ds(z, 1), :] = roll(v, 127 * which - ((z + 1) * TILES + 6))[0:1]
        return result

    def update(w, base, n, stride, xp, edges):
        def at(off):
            return pl.ds(base + off, n, stride=stride) if n > 1 else pl.ds(base + off, 1)

        lanes = lax.broadcasted_iota(jnp.int32, (n, 128), 1)
        member = (lanes & 1) == xp
        stiffness = J[at(0), :]
        local, centre = [], []
        for c in range(2):
            v = S[c, at(0), :]
            edge = edges[c]
            left, right = roll(v, 1), roll(v, -1)
            if xp == 0:
                left = jnp.where(lanes == 0, edge, left)
            else:
                right = jnp.where(lanes == 127, edge, right)
            near = (S[c, at(-1), :] + S[c, at(1), :]) + (S[c, at(-PITCH), :] + S[c, at(PITCH), :]) + (left + right)
            local.append(stiffness * near + K[2 * w + c, at(0), :])
            centre.append(v)
        q = local[0] * local[0] + local[1] * local[1]
        scale = lax.rsqrt(1.0 + q)
        for c in range(2):
            S[c, at(0), :] = jnp.where(member, local[c] * scale, centre[c])
        return q * scale

    def edges_of(z, yp, xp, columns):
        first = 127 * xp - (z + 1) * TILES
        return [jnp.concatenate([roll(columns[c][yp], first - 2 * j) for j in range(3)], axis=0) for c in range(2)]

    def top(w, yp, xp, columns):
        update(w, row(NZ, yp), 24, 2, xp, edges_of(NZ, yp, xp, columns))
        if yp == 0:
            update(w, row(NZ, 48), 1, 1, xp, [XH[2 * xp + c, pl.ds(NZ, 1), :] for c in range(2)])

    def section(w, zp, yp, xp, columns):
        energy = None
        for z in range(zp, NZ, 2):
            e = update(w, row(z, yp), 24, 2, xp, edges_of(z, yp, xp, columns))
            energy = e if energy is None else energy + e
        if yp == 0:
            edges = [XH[2 * xp + c, pl.ds(zp, 8, stride=2), :] for c in range(2)]
            update(w, row(zp, 48), 8, 2 * PITCH, xp, edges)
        energy = energy[0:8] + energy[8:16] + energy[16:24]
        t = 8 * w + 4 * zp + 2 * yp + xp
        EN[t] = jnp.where((lane & 1) == xp, energy, 0.0)

    def sweep(w, copies, recv, table, PR, ES, EJ):
        def arrived(names):
            for name in names:
                if name in copies:
                    copies[name].wait_recv()

        arrived(LEFT + FACES)
        merge_faces(recv, table, w)
        left = spread(0, merge_left(recv, table))
        section(w, 0, 0, 0, left)
        section(w, 0, 1, 0, left)
        arrived(("xZY",) + TOP)
        merge_top(recv, table, w)
        corner = roll(get(recv, table, "xZY", 0), -TILES)
        for c in range(2):
            XH[c, pl.ds(NZ, 1), :] = corner[c : c + 1]
        for yp in range(2):
            top(w, yp, 0, left)
            section(w, 1, yp, 0, left)
        arrived(RIGHT)
        EK, ES, EJ, PM = merge_columns(recv, table, w, PR, ES, EJ)
        ES = update_column(EK, ES, EJ, PM)
        right = spread(1, ES)
        for zp in range(2):
            for yp in range(2):
                if zp == 1:
                    top(w, yp, 1, right)
                section(w, zp, yp, 1, right)
        return ES, EJ

    build(send_a, TABLE_A, 0)
    PJ = pack_first(lambda r: J[pl.ds(r, 8), :])
    PK = [pack_first(lambda r, c=c: K[c, pl.ds(r, 8), :]) for c in range(2)]
    PR = build_columns(send_a, TABLE_A, 0, PJ, PK)
    pl.semaphore_wait(barrier, len(steps))
    for step in ((0, 0, -1), (0, 0, 1)):
        pl.semaphore_signal(token, inc=1, device_id=device(step), device_id_type=MESH)
    for name in [name for name in NAMES if away(name) < 3 and name not in TOP]:
        copies_a[name].start()
    pl.semaphore_wait(token, 2)
    for name in [name for name in NAMES if away(name) == 3] + ["Z", "ZS"]:
        copies_a[name].start()
    loads[3].wait()
    PK = [pack_first(lambda r, c=c: K[2 + c, pl.ds(r, 8), :]) for c in range(2)]
    ES, EJ = sweep(0, copies_a, recv_a, TABLE_A, PR, None, None)

    PR = build_columns(send_b, TABLE_B, 1, PJ, PK)
    build(send_b, TABLE_B, 1)
    for name in NAMES_B:
        copies_b[name].start()
    for name in NAMES:
        copies_a[name].wait_send()
    sweep(1, copies_b, recv_b, TABLE_B, PR, ES, EJ)

    sums = jnp.sum(jnp.sum(EN[...], axis=1), axis=1, keepdims=True)
    diagonal = lax.broadcasted_iota(jnp.int32, (16, 128), 0) == lax.broadcasted_iota(jnp.int32, (16, 128), 1)
    mine = jnp.sum(jnp.where(diagonal, jnp.broadcast_to(sums, (16, 128)), 0.0), axis=0, keepdims=True)
    index = (me[0] * ny + me[1]) * nx + me[2]
    erow[0] = mine
    ebuf[index] = mine

    coords = [[lax.rem(m + d, n) for d in range(n)] for m, n in zip(me, dims)]
    far = [[min(d, n - d) for d in range(n)] for n in dims]
    targets = [(a, b, c) for a in range(nz) for b in range(ny) for c in range(nx) if a + b + c]
    targets.sort(key=lambda t: -(far[0][t[0]] + far[1][t[1]] + (far[2][t[2]] + 1) // 2))
    for a, b, c in targets:
        pltpu.make_async_remote_copy(
            src_ref=erow.at[0],
            dst_ref=ebuf.at[index],
            send_sem=es_sem,
            recv_sem=er_sem,
            device_id=(coords[0][a], coords[1][b], coords[2][c]),
            device_id_type=MESH,
        ).start()
    for z in range(NZ):
        for c in range(2):
            out[c, z] = S[c, pl.ds(row(z, 0), NY), :]
    for name in NAMES_B:
        copies_b[name].wait_send()
    rest = pl.ds(0, total - 1)
    done = pltpu.make_async_remote_copy(
        src_ref=ebuf.at[rest],
        dst_ref=ebuf.at[rest],
        send_sem=es_sem,
        recv_sem=er_sem,
        device_id=me,
        device_id_type=MESH,
    )
    done.wait_recv()
    parts = [ebuf[i] for i in range(8)]
    for i in range(8, total):
        parts[i % 8] = parts[i % 8] + ebuf[i]
    while len(parts) > 1:
        parts = [a + b for a, b in zip(parts[::2], parts[1::2])]
    whole = parts[0]
    sites = float((NZ * nz) * (NY * ny) * (NX * nx) // 8)
    energy_out[...] = (-whole / sites)[0, :16]
    done.wait_send()


def body(dims, spins, kicks, stiffness):
    hbm = pl.BlockSpec(memory_space=pl.ANY)
    total = dims[0] * dims[1] * dims[2]
    vmem, dma = pltpu.VMEM, pltpu.SemaphoreType.DMA
    final, energy = pl.pallas_call(
        functools.partial(kernel, dims),
        out_shape=(
            jax.ShapeDtypeStruct((2, NZ, NY, NX), F32),
            jax.ShapeDtypeStruct((16,), F32),
        ),
        in_specs=[hbm] * 3,
        out_specs=(pl.BlockSpec(memory_space=vmem), pl.BlockSpec(memory_space=vmem)),
        scratch_shapes=[
            vmem((2, ROWS, 128), F32),
            vmem((ROWS, 128), F32),
            vmem((4, ROWS, 128), F32),
            vmem((4, 24, 128), F32),
            vmem((4, 16, 128), F32),
            vmem((SIZE_A, 128), F32),
            vmem((SIZE_A, 128), F32),
            vmem((SIZE_B, 128), F32),
            vmem((SIZE_B, 128), F32),
            vmem((16, 8, 128), F32),
            vmem((total, 1, 128), F32),
            vmem((1, 1, 128), F32),
            dma((4,)),
            pltpu.SemaphoreType.REGULAR,
            dma((COUNT,)),
            dma((COUNT,)),
            dma((COUNT,)),
            dma((COUNT,)),
            dma,
            dma,
        ],
        compiler_params=pltpu.CompilerParams(collective_id=0, has_side_effects=True, vmem_limit_bytes=12 * 1024 * 1024),
    )(*[pltpu.with_memory_space_constraint(v, pltpu.HBM) for v in (spins, kicks, stiffness)])
    def finish(final, energy, out, energy_out, sem):
        copies = [pltpu.make_async_copy(final, out, sem.at[0]), pltpu.make_async_copy(energy, energy_out, sem.at[1])]
        for copy in copies:
            copy.start()
        for copy in copies:
            copy.wait()

    final, energy = [pltpu.with_memory_space_constraint(v, pltpu.VMEM) for v in (final, energy)]
    return pl.pallas_call(
        finish,
        out_shape=(jax.ShapeDtypeStruct((2, NZ, NY, NX), F32), jax.ShapeDtypeStruct((16,), F32)),
        in_specs=[hbm, hbm],
        out_specs=(hbm, hbm),
        scratch_shapes=[dma((2,))],
        compiler_params=pltpu.CompilerParams(vmem_limit_bytes=1024 * 1024),
    )(final, energy)


def solution(mesh):
    dims = tuple(mesh.shape[a] for a in ("gz", "gy", "gx"))
    return jax.shard_map(
        functools.partial(body, dims),
        mesh=mesh,
        in_specs=(P(None, "gz", "gy", "gx"), P(None, None, "gz", "gy", "gx"), P("gz", "gy", "gx")),
        out_specs=(P(None, "gz", "gy", "gx"), P()),
        check_vma=False,
    )
```

```python
import functools

import jax
import jax.numpy as jnp
from jax import lax
from jax.experimental import pallas as pl
from jax.experimental.pallas import tpu as pltpu
from jax.sharding import PartitionSpec as P

MESH = pl.DeviceIdType.MESH
F32 = jnp.float32
NZ, NY, NX = 16, 48, 128
PITCH = 56
ROWS = 19 * PITCH
TILES = 7

MESSAGES = {
    "XZY": ((-1, -1, -1), 8, 8),
    "XZy": ((-1, 1, -1), 8, 8),
    "XzY": ((1, -1, -1), 8, 8),
    "xZY": ((-1, -1, 1), 8, 8),
    "ZY": ((-1, -1, 0), 8, 8),
    "Zy": ((-1, 1, 0), 8, 8),
    "zY": ((1, -1, 0), 8, 8),
    "XZ": ((-1, 0, -1), 8, 8),
    "XY": ((0, -1, -1), 8, 8),
    "Xz": ((1, 0, -1), 8, 8),
    "Xy": ((0, 1, -1), 8, 8),
    "xZ": ((-1, 0, 1), 8, 8),
    "xY": ((0, -1, 1), 8, 8),
    "PZ": ((-1, 0, 0), 8, 8),
    "PY": ((0, -1, 0), 8, 8),
    "X": ((0, 0, -1), 40, 16),
    "x": ((0, 0, 1), 16, 16),
    "z": ((1, 0, 0), 96, 96),
    "Y": ((0, -1, 0), 80, 32),
    "y": ((0, 1, 0), 32, 32),
    "Z": ((-1, 0, 0), 96, 96),
    "ZS": ((-1, 0, 0), 144, 0),
}
NAMES = list(MESSAGES)
COUNT = len(NAMES)
TOP = ("Z", "ZS")
FACES = ("Zy", "zY", "z", "Y", "y")
LEFT = ("x", "xZ", "xY", "ZY")
RIGHT = [name for name in NAMES if name not in FACES + TOP + LEFT + ("xZY",)]
NAMES_B = [name for name in NAMES if name != "ZS"]


def away(name):
    return sum(abs(d) for d in MESSAGES[name][0])


def offsets(round_index):
    start, table = 0, {}
    for name in NAMES:
        size = MESSAGES[name][1 + round_index]
        table[name] = (start, size)
        start += size
    return table, start


TABLE_A, SIZE_A = offsets(0)
TABLE_B, SIZE_B = offsets(1)


def row(z, y):
    return (z + 1) * PITCH + y


def roll(v, shift, axis=1):
    shift = shift % v.shape[axis]
    return v if shift == 0 else pltpu.roll(v, shift, axis)


def kernel(dims, spins, kicks, stiff, out, energy_out, S, J, K, XH, fold, send_a, recv_a, send_b, recv_b, EN, ebuf, erow,
           load_sem, token, sa_sem, ra_sem, sb_sem, rb_sem, es_sem, er_sem):
    nz, ny, nx = dims
    total = nz * ny * nx
    me = (lax.axis_index("gz"), lax.axis_index("gy"), lax.axis_index("gx"))

    def device(step):
        return tuple(lax.rem(m + (d % n), n) for m, d, n in zip(me, step, dims))

    lane = lax.broadcasted_iota(jnp.int32, (8, 128), 1)
    sub = lax.broadcasted_iota(jnp.int32, (8, 128), 0)
    zi = (lane * 9363) >> 16
    tile = lane - zi * 7

    inner = (pl.ds(1, NZ), pl.ds(0, NY))
    planes = ROWS // PITCH
    loads = [
        pltpu.make_async_copy(spins, S.reshape(2, planes, PITCH, 128).at[(slice(None),) + inner], load_sem.at[0]),
        pltpu.make_async_copy(stiff, J.reshape(planes, PITCH, 128).at[inner], load_sem.at[1]),
    ]
    for w in range(2):
        whole = K.reshape(4, planes, PITCH, 128)
        loads.append(pltpu.make_async_copy(kicks.at[w], whole.at[(pl.ds(2 * w, 2),) + inner], load_sem.at[2 + w]))
    for copy in loads:
        copy.start()

    barrier = pltpu.get_barrier_semaphore()
    steps = sorted({MESSAGES[name][0] for name in NAMES if away(name) < 3})
    steps += [(0, 0, d) for d in range(2, nx - 1)]
    steps.sort(key=lambda step: -sum(map(abs, step)))
    for s in steps:
        pl.semaphore_signal(barrier, inc=1, device_id=device(tuple(-d for d in s)), device_id_type=MESH)

    for copy in loads[:3]:
        copy.wait()

    zero_plane = jnp.zeros((PITCH, 128), F32)
    for c in range(2):
        S[c, pl.ds(18 * PITCH, PITCH), :] = zero_plane
        S[c, pl.ds(row(0, 49), NZ, stride=PITCH), :] = jnp.zeros((NZ, 128), F32)
        S[c, pl.ds(row(16, 49), 1), :] = jnp.zeros((1, 128), F32)

    lane3 = lane - ((lane * 21846) >> 16) * 3
    group = [((lane - r + 1) * 21846) >> 16 for r in range(3)]
    own_tiles = [(z + 1) * TILES + t for z in range(NZ) for t in range(6)]

    def pack_spins():
        cols = []
        for c in range(2):
            acc = [jnp.zeros((8, 128), F32) for _ in range(3)]
            for q in own_tiles:
                r = q % 3
                v = roll(S[c, pl.ds(8 * q, 8), :], q)
                acc[r] = jnp.where(group[r] == q // 3, v, acc[r])

            def pick(shift):
                a = [roll(v, shift) for v in acc]
                return jnp.where(lane3 == 0, a[0], jnp.where(lane3 == 1, a[1], a[2]))

            cols.append((pick(0), pick(-1), pick(1)))
        return [[cols[c][k] for c in range(2)] for k in range(3)]

    def pack_first(read):
        acc = jnp.zeros((8, 128), F32)
        for q in own_tiles:
            acc = jnp.where(lane == q, roll(read(8 * q), q), acc)
        return acc

    def zplus(v):
        return roll(v, -7)

    def yplus(v):
        return roll(v, -1, 0)

    def copies(send, recv, table, ssem, rsem):
        result = {}
        for i, name in enumerate(NAMES):
            start, size = table[name]
            if size == 0:
                continue
            part = pl.ds(start, size)
            result[name] = pltpu.make_async_remote_copy(
                src_ref=send.at[part, :],
                dst_ref=recv.at[part, :],
                send_sem=ssem.at[i],
                recv_sem=rsem.at[i],
                device_id=device(MESSAGES[name][0]),
                device_id_type=MESH,
            )
        return result

    def put(send, table, name, at, value):
        send[pl.ds(table[name][0] + at, value.shape[0]), :] = value

    def get(recv, table, name, at, size=8):
        return recv[pl.ds(table[name][0] + at, size), :]

    copies_a = copies(send_a, recv_a, TABLE_A, sa_sem, ra_sem)
    copies_b = copies(send_b, recv_b, TABLE_B, sb_sem, rb_sem)

    def build(send, table, w):
        first = w == 0
        n = 5 if first else 2
        J0 = J[pl.ds(row(0, 0), NY), :]
        for c in range(2):
            kc = K[2 * w + c, pl.ds(row(0, 0), NY), :] + J0 * S[c, pl.ds(row(1, 0), NY), :]
            put(send, table, "Z", c * NY, kc)
            if first:
                put(send, table, "ZS", c * NY, S[c, pl.ds(row(0, 0), NY), :])
            put(send, table, "z", c * NY, S[c, pl.ds(row(15, 0), NY), :])
        if first:
            put(send, table, "ZS", 2 * NY, J0)
        rows0 = pl.ds(row(0, 0), NZ, stride=PITCH)
        rows1 = pl.ds(row(0, 1), NZ, stride=PITCH)
        rows47 = pl.ds(row(0, 47), NZ, stride=PITCH)
        Jy = J[rows0, :]
        for c in range(2):
            kc = K[2 * w + c, rows0, :] + Jy * S[c, rows1, :]
            put(send, table, "Y", (n - 2 + c) * NZ, kc)
            if first:
                put(send, table, "Y", c * NZ, S[c, rows0, :])
            put(send, table, "y", c * NZ, S[c, rows47, :])
        if first:
            put(send, table, "Y", 2 * NZ, Jy)
        at = pl.ds(row(0, 0), 1)
        for c in range(2):
            kc = K[2 * w + c, at, :] + J[at, :] * (S[c, pl.ds(row(1, 0), 1), :] + S[c, pl.ds(row(0, 1), 1), :])
            put(send, table, "ZY", n - 2 + c, kc)
            if first:
                put(send, table, "ZY", c, S[c, at, :])
            put(send, table, "Zy", c, S[c, pl.ds(row(0, 47), 1), :])
            put(send, table, "zY", c, S[c, pl.ds(row(15, 0), 1), :])
        if first:
            put(send, table, "ZY", 2, J[at, :])

    def by_lanes(values, shift=0):
        acc = values[0]
        for k in range(1, len(values)):
            acc = jnp.where((lane >> 4) == k, roll(values[k], 16 * k), acc)
        return acc

    def by_rows(values):
        acc = values[0]
        for k in range(1, len(values)):
            acc = jnp.where(sub == k, roll(values[k], k, 0), acc)
        return acc

    def build_columns(send, table, w, PJ, PK):
        first = w == 0
        PS, PT, PR = pack_spins()
        parts = {name: [] for name in ("X", "XZ", "XY", "XZY")}
        for c in range(2):
            zs, ys = zplus(PS[c]), yplus(PS[c])
            sums = {"X": PT[c], "XZ": PT[c] + zs, "XY": PT[c] + ys, "XZY": PT[c] + zs + ys}
            for name, value in sums.items():
                parts[name].append(PK[c] + PJ * value)
        if first:
            parts = {name: PS + [PJ] + value for name, value in parts.items()}
        put(send, table, "XZY", 0, by_rows(parts["XZY"]))
        put(send, table, "XZ", 0, by_lanes(parts["XZ"]))
        put(send, table, "XY", 0, by_rows(parts["XY"]))
        for k, value in enumerate(parts["X"]):
            put(send, table, "X", 8 * k, value)
        last = jnp.where(sub == 6, roll(PS[1], -1, 0), PS[0])
        put(send, table, "XZy", 0, last)
        put(send, table, "Xy", 0, last)
        put(send, table, "XzY", 0, by_rows(PS))
        put(send, table, "Xz", 0, jnp.where((lane >> 4) == 6, roll(PS[1], -16), PS[0]))
        rows, lanes = by_rows(PR), by_lanes(PR)
        for name in ("xZY", "xY", "PY"):
            put(send, table, name, 0, rows)
        for name in ("xZ", "PZ"):
            put(send, table, name, 0, lanes)
        put(send, table, "ZY", 5, rows[0:2])
        for c in range(2):
            put(send, table, "x", 8 * c, PR[c])
        return PR

    def merge_faces(recv, table, w):
        first = w == 0
        n = 5 if first else 2
        rows48 = pl.ds(row(0, 48), NZ, stride=PITCH)
        at = pl.ds(row(16, 48), 1)
        for c in range(2):
            K[2 * w + c, rows48, :] = get(recv, table, "Y", (n - 2 + c) * NZ, NZ)
            K[2 * w + c, at, :] = get(recv, table, "ZY", n - 2 + c, 1)
            if first:
                S[c, rows48, :] = get(recv, table, "Y", c * NZ, NZ)
                S[c, at, :] = get(recv, table, "ZY", c, 1)
            S[c, pl.ds(row(-1, 0), NY), :] = get(recv, table, "z", c * NY, NY)
            S[c, pl.ds(row(0, -1), NZ, stride=PITCH), :] = get(recv, table, "y", c * NZ, NZ)
            S[c, pl.ds(row(16, -1), 1), :] = get(recv, table, "Zy", c, 1)
            S[c, pl.ds(row(-1, 48), 1), :] = get(recv, table, "zY", c, 1)
        if first:
            J[rows48, :] = get(recv, table, "Y", 2 * NZ, NZ)
            J[at, :] = get(recv, table, "ZY", 2, 1)

    def merge_top(recv, table, w):
        plane = pl.ds(row(16, 0), NY)
        for c in range(2):
            K[2 * w + c, plane, :] = get(recv, table, "Z", c * NY, NY)
            if w == 0:
                S[c, plane, :] = get(recv, table, "ZS", c * NY, NY)
        if w == 0:
            J[plane, :] = get(recv, table, "ZS", 2 * NY, NY)

    at_z = (zi == 17) & (tile < 6)
    at_y = (tile == 6) & (sub == 0) & (zi >= 1) & (zi <= 16)
    at_zy = (zi == 17) & (tile == 6) & (sub == 0)
    at_zm = (zi == 0) & (tile < 6)
    at_ym = (tile == 6) & (sub == 7) & (zi <= 15)
    at_zym = (lane == 118) & (sub == 7)
    at_yzm = (lane == 6) & (sub == 0)

    def upper(base, k, vz, vy, vzy, kzy=None):
        kzy = k if kzy is None else kzy
        base = jnp.where(at_z, roll(vz, 112 - 16 * k), base)
        base = jnp.where(at_y, roll(roll(vy, -k, 0), 6), base)
        return jnp.where(at_zy, roll(roll(vzy, -kzy, 0), 118), base)

    def lower(base, recv, table, c):
        base = jnp.where(at_zm, roll(get(recv, table, "Xz", 0), -112 + 16 * c), base)
        base = jnp.where(at_ym, roll(roll(get(recv, table, "Xy", 0), c, 0), -6), base)
        base = jnp.where(at_zym, roll(roll(get(recv, table, "XZy", 0), c, 0), 106), base)
        return jnp.where(at_yzm, roll(roll(get(recv, table, "XzY", 0), -c, 0), -106), base)

    def merge_left(recv, table):
        result = []
        for c in range(2):
            base = get(recv, table, "x", 8 * c)
            base = jnp.where(at_z, roll(get(recv, table, "xZ", 0), 112 - 16 * c), base)
            result.append(jnp.where(at_y, roll(roll(get(recv, table, "xY", 0), -c, 0), 6), base))
        return result

    def merge_columns(recv, table, w, PR, ES, EJ):
        first = w == 0
        n = 5 if first else 2

        def ext(k):
            base = get(recv, table, "X", 8 * k)
            return upper(base, k, *[get(recv, table, name, 0) for name in ("XZ", "XY", "XZY")])

        EK = [ext(n - 2 + c) for c in range(2)]
        if first:
            ES = [ext(c) for c in range(2)]
            EJ = ext(2)
        ES = [lower(ES[c], recv, table, c) for c in range(2)]
        PM = [upper(PR[c], c, *[get(recv, table, name, 0) for name in ("PZ", "PY", "ZY")], kzy=5 + c) for c in range(2)]
        return EK, ES, EJ, PM

    def shift_up(v):
        v = roll(v, 1, 0)
        return jnp.where(sub == 0, roll(v, 1), v)

    def shift_down(v):
        v = roll(v, -1, 0)
        return jnp.where(sub == 7, roll(v, -1), v)

    inside = (zi >= 1) & (zi <= 17) & ((tile < 6) | (sub == 0))

    def update_column(EK, ES, EJ, PM):
        for zp in range(2):
            for yp in range(2):
                member = inside & ((zi & 1) == 1 - zp) & ((sub & 1) == yp)
                local = []
                for c in range(2):
                    v = ES[c]
                    above = jnp.where(lane < 17 * TILES, roll(v, -7), 0.0)
                    near = shift_up(v) + shift_down(v) + roll(v, 7) + above + PM[c]
                    local.append(EJ * near + EK[c])
                scale = lax.rsqrt(1.0 + (local[0] * local[0] + local[1] * local[1]))
                ES = [jnp.where(member, local[c] * scale, ES[c]) for c in range(2)]
        return ES

    def spread(which, values):
        result = []
        for c in range(2):
            v = values[c]
            fold[2 * which + c, 0:8] = v
            fold[2 * which + c, 8:16] = roll(v, -1)
            result.append([fold[2 * which + c, pl.ds(yp, 8, stride=2)] for yp in range(2)])
            for z in range(NZ + which):
                XH[2 * which + c, pl.ds(z, 1), :] = roll(v, 127 * which - ((z + 1) * TILES + 6))[0:1]
        return result

    def update(w, base, n, stride, xp, edges):
        def at(off):
            return pl.ds(base + off, n, stride=stride) if n > 1 else pl.ds(base + off, 1)

        lanes = lax.broadcasted_iota(jnp.int32, (n, 128), 1)
        member = (lanes & 1) == xp
        stiffness = J[at(0), :]
        local, centre = [], []
        for c in range(2):
            v = S[c, at(0), :]
            edge = edges[c]
            left, right = roll(v, 1), roll(v, -1)
            if xp == 0:
                left = jnp.where(lanes == 0, edge, left)
            else:
                right = jnp.where(lanes == 127, edge, right)
            near = (S[c, at(-1), :] + S[c, at(1), :]) + (S[c, at(-PITCH), :] + S[c, at(PITCH), :]) + (left + right)
            local.append(stiffness * near + K[2 * w + c, at(0), :])
            centre.append(v)
        q = local[0] * local[0] + local[1] * local[1]
        scale = lax.rsqrt(1.0 + q)
        for c in range(2):
            S[c, at(0), :] = jnp.where(member, local[c] * scale, centre[c])
        return q * scale

    def edges_of(z, yp, xp, columns):
        first = 127 * xp - (z + 1) * TILES
        return [jnp.concatenate([roll(columns[c][yp], first - 2 * j) for j in range(3)], axis=0) for c in range(2)]

    def top(w, yp, xp, columns):
        update(w, row(NZ, yp), 24, 2, xp, edges_of(NZ, yp, xp, columns))
        if yp == 0:
            update(w, row(NZ, 48), 1, 1, xp, [XH[2 * xp + c, pl.ds(NZ, 1), :] for c in range(2)])

    def section(w, zp, yp, xp, columns):
        energy = None
        for z in range(zp, NZ, 2):
            e = update(w, row(z, yp), 24, 2, xp, edges_of(z, yp, xp, columns))
            energy = e if energy is None else energy + e
        if yp == 0:
            edges = [XH[2 * xp + c, pl.ds(zp, 8, stride=2), :] for c in range(2)]
            update(w, row(zp, 48), 8, 2 * PITCH, xp, edges)
        energy = energy[0:8] + energy[8:16] + energy[16:24]
        t = 8 * w + 4 * zp + 2 * yp + xp
        EN[t] = jnp.where((lane & 1) == xp, energy, 0.0)

    def sweep(w, copies, recv, table, PR, ES, EJ):
        def arrived(names):
            for name in names:
                if name in copies:
                    copies[name].wait_recv()

        arrived(LEFT + FACES)
        arrived(RIGHT)
        EK, ES, EJ, PM = merge_columns(recv, table, w, PR, ES, EJ)
        ES = update_column(EK, ES, EJ, PM)
        right = spread(1, ES)
        merge_faces(recv, table, w)
        left = spread(0, merge_left(recv, table))
        section(w, 0, 0, 0, left)
        section(w, 0, 1, 0, left)
        arrived(("xZY",) + TOP)
        merge_top(recv, table, w)
        corner = roll(get(recv, table, "xZY", 0), -TILES)
        for c in range(2):
            XH[c, pl.ds(NZ, 1), :] = corner[c : c + 1]
        for yp in range(2):
            top(w, yp, 0, left)
            section(w, 1, yp, 0, left)
        for zp in range(2):
            for yp in range(2):
                if zp == 1:
                    top(w, yp, 1, right)
                section(w, zp, yp, 1, right)
        return ES, EJ

    build(send_a, TABLE_A, 0)
    PJ = pack_first(lambda r: J[pl.ds(r, 8), :])
    PK = [pack_first(lambda r, c=c: K[c, pl.ds(r, 8), :]) for c in range(2)]
    PR = build_columns(send_a, TABLE_A, 0, PJ, PK)
    pl.semaphore_wait(barrier, len(steps))
    for step in ((0, 0, -1), (0, 0, 1)):
        pl.semaphore_signal(token, inc=1, device_id=device(step), device_id_type=MESH)
    for name in [name for name in NAMES if away(name) < 3 and name not in TOP]:
        copies_a[name].start()
    pl.semaphore_wait(token, 2)
    for name in [name for name in NAMES if away(name) == 3] + ["Z", "ZS"]:
        copies_a[name].start()
    loads[3].wait()
    PK = [pack_first(lambda r, c=c: K[2 + c, pl.ds(r, 8), :]) for c in range(2)]
    ES, EJ = sweep(0, copies_a, recv_a, TABLE_A, PR, None, None)

    PR = build_columns(send_b, TABLE_B, 1, PJ, PK)
    build(send_b, TABLE_B, 1)
    for name in NAMES_B:
        copies_b[name].start()
    for name in NAMES:
        copies_a[name].wait_send()
    sweep(1, copies_b, recv_b, TABLE_B, PR, ES, EJ)

    sums = jnp.sum(jnp.sum(EN[...], axis=1), axis=1, keepdims=True)
    diagonal = lax.broadcasted_iota(jnp.int32, (16, 128), 0) == lax.broadcasted_iota(jnp.int32, (16, 128), 1)
    mine = jnp.sum(jnp.where(diagonal, jnp.broadcast_to(sums, (16, 128)), 0.0), axis=0, keepdims=True)
    index = (me[0] * ny + me[1]) * nx + me[2]
    erow[0] = mine
    ebuf[index] = mine

    coords = [[lax.rem(m + d, n) for d in range(n)] for m, n in zip(me, dims)]
    far = [[min(d, n - d) for d in range(n)] for n in dims]
    targets = [(a, b, c) for a in range(nz) for b in range(ny) for c in range(nx) if a + b + c]
    targets.sort(key=lambda t: -(far[0][t[0]] + far[1][t[1]] + (far[2][t[2]] + 1) // 2))
    for a, b, c in targets:
        pltpu.make_async_remote_copy(
            src_ref=erow.at[0],
            dst_ref=ebuf.at[index],
            send_sem=es_sem,
            recv_sem=er_sem,
            device_id=(coords[0][a], coords[1][b], coords[2][c]),
            device_id_type=MESH,
        ).start()
    for z in range(NZ):
        for c in range(2):
            out[c, z] = S[c, pl.ds(row(z, 0), NY), :]
    for name in NAMES_B:
        copies_b[name].wait_send()
    rest = pl.ds(0, total - 1)
    done = pltpu.make_async_remote_copy(
        src_ref=ebuf.at[rest],
        dst_ref=ebuf.at[rest],
        send_sem=es_sem,
        recv_sem=er_sem,
        device_id=me,
        device_id_type=MESH,
    )
    done.wait_recv()
    parts = [ebuf[i] for i in range(8)]
    for i in range(8, total):
        parts[i % 8] = parts[i % 8] + ebuf[i]
    while len(parts) > 1:
        parts = [a + b for a, b in zip(parts[::2], parts[1::2])]
    whole = parts[0]
    sites = float((NZ * nz) * (NY * ny) * (NX * nx) // 8)
    energy_out[...] = (-whole / sites)[0, :16]
    done.wait_send()


def body(dims, spins, kicks, stiffness):
    hbm = pl.BlockSpec(memory_space=pl.ANY)
    total = dims[0] * dims[1] * dims[2]
    vmem, dma = pltpu.VMEM, pltpu.SemaphoreType.DMA
    final, energy = pl.pallas_call(
        functools.partial(kernel, dims),
        out_shape=(
            jax.ShapeDtypeStruct((2, NZ, NY, NX), F32),
            jax.ShapeDtypeStruct((16,), F32),
        ),
        in_specs=[hbm] * 3,
        out_specs=(pl.BlockSpec(memory_space=vmem), pl.BlockSpec(memory_space=vmem)),
        scratch_shapes=[
            vmem((2, ROWS, 128), F32),
            vmem((ROWS, 128), F32),
            vmem((4, ROWS, 128), F32),
            vmem((4, 24, 128), F32),
            vmem((4, 16, 128), F32),
            vmem((SIZE_A, 128), F32),
            vmem((SIZE_A, 128), F32),
            vmem((SIZE_B, 128), F32),
            vmem((SIZE_B, 128), F32),
            vmem((16, 8, 128), F32),
            vmem((total, 1, 128), F32),
            vmem((1, 1, 128), F32),
            dma((4,)),
            pltpu.SemaphoreType.REGULAR,
            dma((COUNT,)),
            dma((COUNT,)),
            dma((COUNT,)),
            dma((COUNT,)),
            dma,
            dma,
        ],
        compiler_params=pltpu.CompilerParams(collective_id=0, has_side_effects=True, vmem_limit_bytes=12 * 1024 * 1024),
    )(*[pltpu.with_memory_space_constraint(v, pltpu.HBM) for v in (spins, kicks, stiffness)])
    def finish(final, energy, out, energy_out, sem):
        copies = [pltpu.make_async_copy(final, out, sem.at[0]), pltpu.make_async_copy(energy, energy_out, sem.at[1])]
        for copy in copies:
            copy.start()
        for copy in copies:
            copy.wait()

    final, energy = [pltpu.with_memory_space_constraint(v, pltpu.VMEM) for v in (final, energy)]
    return pl.pallas_call(
        finish,
        out_shape=(jax.ShapeDtypeStruct((2, NZ, NY, NX), F32), jax.ShapeDtypeStruct((16,), F32)),
        in_specs=[hbm, hbm],
        out_specs=(hbm, hbm),
        scratch_shapes=[dma((2,))],
        compiler_params=pltpu.CompilerParams(vmem_limit_bytes=1024 * 1024),
    )(final, energy)


def solution(mesh):
    dims = tuple(mesh.shape[a] for a in ("gz", "gy", "gx"))
    return jax.shard_map(
        functools.partial(body, dims),
        mesh=mesh,
        in_specs=(P(None, "gz", "gy", "gx"), P(None, None, "gz", "gy", "gx"), P("gz", "gy", "gx")),
        out_specs=(P(None, "gz", "gy", "gx"), P()),
        check_vma=False,
    )
```

```python
import functools

import jax
import jax.numpy as jnp
from jax import lax
from jax.experimental import pallas as pl
from jax.experimental.pallas import tpu as pltpu
from jax.sharding import PartitionSpec as P

MESH = pl.DeviceIdType.MESH
F32 = jnp.float32
NZ, NY, NX = 16, 48, 128
PITCH = 56
ROWS = 19 * PITCH
TILES = 7

MESSAGES = {
    "XZY": ((-1, -1, -1), 8, 8),
    "XZy": ((-1, 1, -1), 8, 8),
    "XzY": ((1, -1, -1), 8, 8),
    "xZY": ((-1, -1, 1), 8, 8),
    "ZY": ((-1, -1, 0), 8, 8),
    "Zy": ((-1, 1, 0), 8, 8),
    "zY": ((1, -1, 0), 8, 8),
    "XZ": ((-1, 0, -1), 8, 8),
    "XY": ((0, -1, -1), 8, 8),
    "Xz": ((1, 0, -1), 8, 8),
    "Xy": ((0, 1, -1), 8, 8),
    "xZ": ((-1, 0, 1), 8, 8),
    "xY": ((0, -1, 1), 8, 8),
    "PZ": ((-1, 0, 0), 8, 8),
    "PY": ((0, -1, 0), 8, 8),
    "X": ((0, 0, -1), 40, 16),
    "x": ((0, 0, 1), 16, 16),
    "z": ((1, 0, 0), 96, 96),
    "Y": ((0, -1, 0), 80, 32),
    "y": ((0, 1, 0), 32, 32),
    "Z": ((-1, 0, 0), 96, 96),
    "ZS": ((-1, 0, 0), 144, 0),
}
NAMES = list(MESSAGES)
COUNT = len(NAMES)
TOP = ("Z", "ZS")
FACES = ("Zy", "zY", "z", "Y", "y")
LEFT = ("x", "xZ", "xY", "ZY")
RIGHT = [name for name in NAMES if name not in FACES + TOP + LEFT + ("xZY",)]
NAMES_B = [name for name in NAMES if name != "ZS"]


def away(name):
    return sum(abs(d) for d in MESSAGES[name][0])


def offsets(round_index):
    start, table = 0, {}
    for name in NAMES:
        size = MESSAGES[name][1 + round_index]
        table[name] = (start, size)
        start += size
    return table, start


TABLE_A, SIZE_A = offsets(0)
TABLE_B, SIZE_B = offsets(1)


def row(z, y):
    return (z + 1) * PITCH + y


def roll(v, shift, axis=1):
    shift = shift % v.shape[axis]
    return v if shift == 0 else pltpu.roll(v, shift, axis)


def kernel(dims, spins, kicks, stiff, out, energy_out, S, J, K, XH, fold, send_a, recv_a, send_b, recv_b, EN, ebuf, erow,
           load_sem, token, sa_sem, ra_sem, sb_sem, rb_sem, es_sem, er_sem):
    nz, ny, nx = dims
    total = nz * ny * nx
    me = (lax.axis_index("gz"), lax.axis_index("gy"), lax.axis_index("gx"))

    def device(step):
        return tuple(lax.rem(m + (d % n), n) for m, d, n in zip(me, step, dims))

    lane = lax.broadcasted_iota(jnp.int32, (8, 128), 1)
    sub = lax.broadcasted_iota(jnp.int32, (8, 128), 0)
    zi = (lane * 9363) >> 16
    tile = lane - zi * 7

    inner = (pl.ds(1, NZ), pl.ds(0, NY))
    planes = ROWS // PITCH
    loads = [
        pltpu.make_async_copy(spins, S.reshape(2, planes, PITCH, 128).at[(slice(None),) + inner], load_sem.at[0]),
        pltpu.make_async_copy(stiff, J.reshape(planes, PITCH, 128).at[inner], load_sem.at[1]),
    ]
    for w in range(2):
        whole = K.reshape(4, planes, PITCH, 128)
        loads.append(pltpu.make_async_copy(kicks.at[w], whole.at[(pl.ds(2 * w, 2),) + inner], load_sem.at[2 + w]))
    for copy in loads:
        copy.start()

    barrier = pltpu.get_barrier_semaphore()
    steps = sorted({MESSAGES[name][0] for name in NAMES if away(name) < 3})
    steps += [(0, 0, d) for d in range(2, nx - 1)]
    steps.sort(key=lambda step: -sum(map(abs, step)))
    for s in steps:
        pl.semaphore_signal(barrier, inc=1, device_id=device(tuple(-d for d in s)), device_id_type=MESH)

    for copy in loads[:3]:
        copy.wait()

    zero_plane = jnp.zeros((PITCH, 128), F32)
    for c in range(2):
        S[c, pl.ds(18 * PITCH, PITCH), :] = zero_plane
        S[c, pl.ds(row(0, 49), NZ, stride=PITCH), :] = jnp.zeros((NZ, 128), F32)
        S[c, pl.ds(row(16, 49), 1), :] = jnp.zeros((1, 128), F32)

    lane3 = lane - ((lane * 21846) >> 16) * 3
    group = [((lane - r + 1) * 21846) >> 16 for r in range(3)]
    own_tiles = [(z + 1) * TILES + t for z in range(NZ) for t in range(6)]

    def pack_spins():
        cols = []
        for c in range(2):
            acc = [jnp.zeros((8, 128), F32) for _ in range(3)]
            for q in own_tiles:
                r = q % 3
                v = roll(S[c, pl.ds(8 * q, 8), :], q)
                acc[r] = jnp.where(group[r] == q // 3, v, acc[r])

            def pick(shift):
                a = [roll(v, shift) for v in acc]
                return jnp.where(lane3 == 0, a[0], jnp.where(lane3 == 1, a[1], a[2]))

            cols.append((pick(0), pick(-1), pick(1)))
        return [[cols[c][k] for c in range(2)] for k in range(3)]

    def pack_first(read):
        acc = jnp.zeros((8, 128), F32)
        for q in own_tiles:
            acc = jnp.where(lane == q, roll(read(8 * q), q), acc)
        return acc

    def zplus(v):
        return roll(v, -7)

    def yplus(v):
        return roll(v, -1, 0)

    def copies(send, recv, table, ssem, rsem):
        result = {}
        for i, name in enumerate(NAMES):
            start, size = table[name]
            if size == 0:
                continue
            part = pl.ds(start, size)
            result[name] = pltpu.make_async_remote_copy(
                src_ref=send.at[part, :],
                dst_ref=recv.at[part, :],
                send_sem=ssem.at[i],
                recv_sem=rsem.at[i],
                device_id=device(MESSAGES[name][0]),
                device_id_type=MESH,
            )
        return result

    def put(send, table, name, at, value):
        send[pl.ds(table[name][0] + at, value.shape[0]), :] = value

    def get(recv, table, name, at, size=8):
        return recv[pl.ds(table[name][0] + at, size), :]

    copies_a = copies(send_a, recv_a, TABLE_A, sa_sem, ra_sem)
    copies_b = copies(send_b, recv_b, TABLE_B, sb_sem, rb_sem)

    def build(send, table, w):
        first = w == 0
        n = 5 if first else 2
        J0 = J[pl.ds(row(0, 0), NY), :]
        for c in range(2):
            kc = K[2 * w + c, pl.ds(row(0, 0), NY), :] + J0 * S[c, pl.ds(row(1, 0), NY), :]
            put(send, table, "Z", c * NY, kc)
            if first:
                put(send, table, "ZS", c * NY, S[c, pl.ds(row(0, 0), NY), :])
            put(send, table, "z", c * NY, S[c, pl.ds(row(15, 0), NY), :])
        if first:
            put(send, table, "ZS", 2 * NY, J0)
        rows0 = pl.ds(row(0, 0), NZ, stride=PITCH)
        rows1 = pl.ds(row(0, 1), NZ, stride=PITCH)
        rows47 = pl.ds(row(0, 47), NZ, stride=PITCH)
        Jy = J[rows0, :]
        for c in range(2):
            kc = K[2 * w + c, rows0, :] + Jy * S[c, rows1, :]
            put(send, table, "Y", (n - 2 + c) * NZ, kc)
            if first:
                put(send, table, "Y", c * NZ, S[c, rows0, :])
            put(send, table, "y", c * NZ, S[c, rows47, :])
        if first:
            put(send, table, "Y", 2 * NZ, Jy)
        at = pl.ds(row(0, 0), 1)
        for c in range(2):
            kc = K[2 * w + c, at, :] + J[at, :] * (S[c, pl.ds(row(1, 0), 1), :] + S[c, pl.ds(row(0, 1), 1), :])
            put(send, table, "ZY", n - 2 + c, kc)
            if first:
                put(send, table, "ZY", c, S[c, at, :])
            put(send, table, "Zy", c, S[c, pl.ds(row(0, 47), 1), :])
            put(send, table, "zY", c, S[c, pl.ds(row(15, 0), 1), :])
        if first:
            put(send, table, "ZY", 2, J[at, :])

    def by_lanes(values, shift=0):
        acc = values[0]
        for k in range(1, len(values)):
            acc = jnp.where((lane >> 4) == k, roll(values[k], 16 * k), acc)
        return acc

    def by_rows(values):
        acc = values[0]
        for k in range(1, len(values)):
            acc = jnp.where(sub == k, roll(values[k], k, 0), acc)
        return acc

    def build_columns(send, table, w, PJ, PK):
        first = w == 0
        PS, PT, PR = pack_spins()
        parts = {name: [] for name in ("X", "XZ", "XY", "XZY")}
        for c in range(2):
            zs, ys = zplus(PS[c]), yplus(PS[c])
            sums = {"X": PT[c], "XZ": PT[c] + zs, "XY": PT[c] + ys, "XZY": PT[c] + zs + ys}
            for name, value in sums.items():
                parts[name].append(PK[c] + PJ * value)
        if first:
            parts = {name: PS + [PJ] + value for name, value in parts.items()}
        put(send, table, "XZY", 0, by_rows(parts["XZY"]))
        put(send, table, "XZ", 0, by_lanes(parts["XZ"]))
        put(send, table, "XY", 0, by_rows(parts["XY"]))
        for k, value in enumerate(parts["X"]):
            put(send, table, "X", 8 * k, value)
        last = jnp.where(sub == 6, roll(PS[1], -1, 0), PS[0])
        put(send, table, "XZy", 0, last)
        put(send, table, "Xy", 0, last)
        put(send, table, "XzY", 0, by_rows(PS))
        put(send, table, "Xz", 0, jnp.where((lane >> 4) == 6, roll(PS[1], -16), PS[0]))
        rows, lanes = by_rows(PR), by_lanes(PR)
        for name in ("xZY", "xY", "PY"):
            put(send, table, name, 0, rows)
        for name in ("xZ", "PZ"):
            put(send, table, name, 0, lanes)
        put(send, table, "ZY", 5, rows[0:2])
        for c in range(2):
            put(send, table, "x", 8 * c, PR[c])
        return PR

    def merge_faces(recv, table, w):
        first = w == 0
        n = 5 if first else 2
        rows48 = pl.ds(row(0, 48), NZ, stride=PITCH)
        at = pl.ds(row(16, 48), 1)
        for c in range(2):
            K[2 * w + c, rows48, :] = get(recv, table, "Y", (n - 2 + c) * NZ, NZ)
            K[2 * w + c, at, :] = get(recv, table, "ZY", n - 2 + c, 1)
            if first:
                S[c, rows48, :] = get(recv, table, "Y", c * NZ, NZ)
                S[c, at, :] = get(recv, table, "ZY", c, 1)
            S[c, pl.ds(row(-1, 0), NY), :] = get(recv, table, "z", c * NY, NY)
            S[c, pl.ds(row(0, -1), NZ, stride=PITCH), :] = get(recv, table, "y", c * NZ, NZ)
            S[c, pl.ds(row(16, -1), 1), :] = get(recv, table, "Zy", c, 1)
            S[c, pl.ds(row(-1, 48), 1), :] = get(recv, table, "zY", c, 1)
        if first:
            J[rows48, :] = get(recv, table, "Y", 2 * NZ, NZ)
            J[at, :] = get(recv, table, "ZY", 2, 1)

    def merge_top(recv, table, w):
        plane = pl.ds(row(16, 0), NY)
        for c in range(2):
            K[2 * w + c, plane, :] = get(recv, table, "Z", c * NY, NY)
            if w == 0:
                S[c, plane, :] = get(recv, table, "ZS", c * NY, NY)
        if w == 0:
            J[plane, :] = get(recv, table, "ZS", 2 * NY, NY)

    at_z = (zi == 17) & (tile < 6)
    at_y = (tile == 6) & (sub == 0) & (zi >= 1) & (zi <= 16)
    at_zy = (zi == 17) & (tile == 6) & (sub == 0)
    at_zm = (zi == 0) & (tile < 6)
    at_ym = (tile == 6) & (sub == 7) & (zi <= 15)
    at_zym = (lane == 118) & (sub == 7)
    at_yzm = (lane == 6) & (sub == 0)

    def upper(base, k, vz, vy, vzy, kzy=None):
        kzy = k if kzy is None else kzy
        base = jnp.where(at_z, roll(vz, 112 - 16 * k), base)
        base = jnp.where(at_y, roll(roll(vy, -k, 0), 6), base)
        return jnp.where(at_zy, roll(roll(vzy, -kzy, 0), 118), base)

    def lower(base, recv, table, c):
        base = jnp.where(at_zm, roll(get(recv, table, "Xz", 0), -112 + 16 * c), base)
        base = jnp.where(at_ym, roll(roll(get(recv, table, "Xy", 0), c, 0), -6), base)
        base = jnp.where(at_zym, roll(roll(get(recv, table, "XZy", 0), c, 0), 106), base)
        return jnp.where(at_yzm, roll(roll(get(recv, table, "XzY", 0), -c, 0), -106), base)

    def merge_left(recv, table):
        result = []
        for c in range(2):
            base = get(recv, table, "x", 8 * c)
            base = jnp.where(at_z, roll(get(recv, table, "xZ", 0), 112 - 16 * c), base)
            result.append(jnp.where(at_y, roll(roll(get(recv, table, "xY", 0), -c, 0), 6), base))
        return result

    def merge_columns(recv, table, w, PR, ES, EJ):
        first = w == 0
        n = 5 if first else 2

        def ext(k):
            base = get(recv, table, "X", 8 * k)
            return upper(base, k, *[get(recv, table, name, 0) for name in ("XZ", "XY", "XZY")])

        EK = [ext(n - 2 + c) for c in range(2)]
        if first:
            ES = [ext(c) for c in range(2)]
            EJ = ext(2)
        ES = [lower(ES[c], recv, table, c) for c in range(2)]
        PM = [upper(PR[c], c, *[get(recv, table, name, 0) for name in ("PZ", "PY", "ZY")], kzy=5 + c) for c in range(2)]
        return EK, ES, EJ, PM

    def shift_up(v):
        v = roll(v, 1, 0)
        return jnp.where(sub == 0, roll(v, 1), v)

    def shift_down(v):
        v = roll(v, -1, 0)
        return jnp.where(sub == 7, roll(v, -1), v)

    inside = (zi >= 1) & (zi <= 17) & ((tile < 6) | (sub == 0))

    def update_column(EK, ES, EJ, PM):
        for zp in range(2):
            for yp in range(2):
                member = inside & ((zi & 1) == 1 - zp) & ((sub & 1) == yp)
                local = []
                for c in range(2):
                    v = ES[c]
                    above = jnp.where(lane < 17 * TILES, roll(v, -7), 0.0)
                    near = shift_up(v) + shift_down(v) + roll(v, 7) + above + PM[c]
                    local.append(EJ * near + EK[c])
                scale = lax.rsqrt(1.0 + (local[0] * local[0] + local[1] * local[1]))
                ES = [jnp.where(member, local[c] * scale, ES[c]) for c in range(2)]
        return ES

    def spread(which, values):
        result = []
        for c in range(2):
            v = values[c]
            fold[2 * which + c, 0:8] = v
            fold[2 * which + c, 8:16] = roll(v, -1)
            result.append([fold[2 * which + c, pl.ds(yp, 8, stride=2)] for yp in range(2)])
            for z in range(NZ + which):
                XH[2 * which + c, pl.ds(z, 1), :] = roll(v, 127 * which - ((z + 1) * TILES + 6))[0:1]
        return result

    def update(w, base, n, stride, xp, edges):
        def at(off):
            return pl.ds(base + off, n, stride=stride) if n > 1 else pl.ds(base + off, 1)

        lanes = lax.broadcasted_iota(jnp.int32, (n, 128), 1)
        member = (lanes & 1) == xp
        stiffness = J[at(0), :]
        local, centre = [], []
        for c in range(2):
            v = S[c, at(0), :]
            edge = edges[c]
            left, right = roll(v, 1), roll(v, -1)
            if xp == 0:
                left = jnp.where(lanes == 0, edge, left)
            else:
                right = jnp.where(lanes == 127, edge, right)
            near = (S[c, at(-1), :] + S[c, at(1), :]) + (S[c, at(-PITCH), :] + S[c, at(PITCH), :]) + (left + right)
            local.append(stiffness * near + K[2 * w + c, at(0), :])
            centre.append(v)
        q = local[0] * local[0] + local[1] * local[1]
        scale = lax.rsqrt(1.0 + q)
        for c in range(2):
            S[c, at(0), :] = jnp.where(member, local[c] * scale, centre[c])
        return q * scale

    def edges_of(z, yp, xp, columns):
        first = 127 * xp - (z + 1) * TILES
        return [jnp.concatenate([roll(columns[c][yp], first - 2 * j) for j in range(3)], axis=0) for c in range(2)]

    def top(w, yp, xp, columns):
        update(w, row(NZ, yp), 24, 2, xp, edges_of(NZ, yp, xp, columns))
        if yp == 0:
            update(w, row(NZ, 48), 1, 1, xp, [XH[2 * xp + c, pl.ds(NZ, 1), :] for c in range(2)])

    def section(w, zp, yp, xp, columns):
        energy = None
        for z in range(zp, NZ, 2):
            e = update(w, row(z, yp), 24, 2, xp, edges_of(z, yp, xp, columns))
            energy = e if energy is None else energy + e
        if yp == 0:
            edges = [XH[2 * xp + c, pl.ds(zp, 8, stride=2), :] for c in range(2)]
            update(w, row(zp, 48), 8, 2 * PITCH, xp, edges)
        energy = energy[0:8] + energy[8:16] + energy[16:24]
        t = 8 * w + 4 * zp + 2 * yp + xp
        EN[t] = jnp.where((lane & 1) == xp, energy, 0.0)

    def row_of_sums():
        sums = jnp.sum(jnp.sum(EN[0:15], axis=1), axis=1, keepdims=True)
        lanes = lax.broadcasted_iota(jnp.int32, (15, 128), 1)
        diagonal = lanes == lax.broadcasted_iota(jnp.int32, (15, 128), 0)
        return jnp.sum(jnp.where(diagonal, jnp.broadcast_to(sums, (15, 128)), 0.0), axis=0, keepdims=True)

    def sweep(w, copies, recv, table, PR, ES, EJ):
        def arrived(names):
            for name in names:
                if name in copies:
                    copies[name].wait_recv()

        arrived(LEFT + FACES)
        arrived(RIGHT)
        EK, ES, EJ, PM = merge_columns(recv, table, w, PR, ES, EJ)
        ES = update_column(EK, ES, EJ, PM)
        right = spread(1, ES)
        merge_faces(recv, table, w)
        left = spread(0, merge_left(recv, table))
        section(w, 0, 0, 0, left)
        section(w, 0, 1, 0, left)
        arrived(("xZY",) + TOP)
        merge_top(recv, table, w)
        corner = roll(get(recv, table, "xZY", 0), -TILES)
        for c in range(2):
            XH[c, pl.ds(NZ, 1), :] = corner[c : c + 1]
        for yp in range(2):
            top(w, yp, 0, left)
            section(w, 1, yp, 0, left)
        for zp in range(2):
            for yp in range(2):
                if zp == 1:
                    top(w, yp, 1, right)
                early = row_of_sums() if (w, zp, yp) == (1, 1, 1) else None
                section(w, zp, yp, 1, right)
        return ES, EJ, early

    build(send_a, TABLE_A, 0)
    PJ = pack_first(lambda r: J[pl.ds(r, 8), :])
    PK = [pack_first(lambda r, c=c: K[c, pl.ds(r, 8), :]) for c in range(2)]
    PR = build_columns(send_a, TABLE_A, 0, PJ, PK)
    pl.semaphore_wait(barrier, len(steps))
    for step in ((0, 0, -1), (0, 0, 1)):
        pl.semaphore_signal(token, inc=1, device_id=device(step), device_id_type=MESH)
    for name in [name for name in NAMES if away(name) < 3 and name not in TOP]:
        copies_a[name].start()
    pl.semaphore_wait(token, 2)
    for name in [name for name in NAMES if away(name) == 3] + ["Z", "ZS"]:
        copies_a[name].start()
    loads[3].wait()
    PK = [pack_first(lambda r, c=c: K[2 + c, pl.ds(r, 8), :]) for c in range(2)]
    ES, EJ, _ = sweep(0, copies_a, recv_a, TABLE_A, PR, None, None)

    PR = build_columns(send_b, TABLE_B, 1, PJ, PK)
    build(send_b, TABLE_B, 1)
    for name in NAMES_B:
        copies_b[name].start()
    for name in NAMES:
        copies_a[name].wait_send()
    _, _, early = sweep(1, copies_b, recv_b, TABLE_B, PR, ES, EJ)

    last = jnp.sum(jnp.sum(EN[15], axis=0, keepdims=True), axis=1, keepdims=True)
    mine = jnp.where(lane[0:1] == 15, jnp.broadcast_to(last, (1, 128)), early)
    index = (me[0] * ny + me[1]) * nx + me[2]
    erow[0] = mine
    ebuf[index] = mine

    coords = [[lax.rem(m + d, n) for d in range(n)] for m, n in zip(me, dims)]
    far = [[min(d, n - d) for d in range(n)] for n in dims]
    targets = [(a, b, c) for a in range(nz) for b in range(ny) for c in range(nx) if a + b + c]
    targets.sort(key=lambda t: -(far[0][t[0]] + far[1][t[1]] + (far[2][t[2]] + 1) // 2))
    for a, b, c in targets:
        pltpu.make_async_remote_copy(
            src_ref=erow.at[0],
            dst_ref=ebuf.at[index],
            send_sem=es_sem,
            recv_sem=er_sem,
            device_id=(coords[0][a], coords[1][b], coords[2][c]),
            device_id_type=MESH,
        ).start()
    for z in range(NZ):
        for c in range(2):
            out[c, z] = S[c, pl.ds(row(z, 0), NY), :]
    for name in NAMES_B:
        copies_b[name].wait_send()
    rest = pl.ds(0, total - 1)
    done = pltpu.make_async_remote_copy(
        src_ref=ebuf.at[rest],
        dst_ref=ebuf.at[rest],
        send_sem=es_sem,
        recv_sem=er_sem,
        device_id=me,
        device_id_type=MESH,
    )
    done.wait_recv()
    parts = [ebuf[i] for i in range(8)]
    for i in range(8, total):
        parts[i % 8] = parts[i % 8] + ebuf[i]
    while len(parts) > 1:
        parts = [a + b for a, b in zip(parts[::2], parts[1::2])]
    whole = parts[0]
    sites = float((NZ * nz) * (NY * ny) * (NX * nx) // 8)
    energy_out[...] = (-whole / sites)[0, :16]
    done.wait_send()


def body(dims, spins, kicks, stiffness):
    hbm = pl.BlockSpec(memory_space=pl.ANY)
    total = dims[0] * dims[1] * dims[2]
    vmem, dma = pltpu.VMEM, pltpu.SemaphoreType.DMA
    final, energy = pl.pallas_call(
        functools.partial(kernel, dims),
        out_shape=(
            jax.ShapeDtypeStruct((2, NZ, NY, NX), F32),
            jax.ShapeDtypeStruct((16,), F32),
        ),
        in_specs=[hbm] * 3,
        out_specs=(pl.BlockSpec(memory_space=vmem), pl.BlockSpec(memory_space=vmem)),
        scratch_shapes=[
            vmem((2, ROWS, 128), F32),
            vmem((ROWS, 128), F32),
            vmem((4, ROWS, 128), F32),
            vmem((4, 24, 128), F32),
            vmem((4, 16, 128), F32),
            vmem((SIZE_A, 128), F32),
            vmem((SIZE_A, 128), F32),
            vmem((SIZE_B, 128), F32),
            vmem((SIZE_B, 128), F32),
            vmem((16, 8, 128), F32),
            vmem((total, 1, 128), F32),
            vmem((1, 1, 128), F32),
            dma((4,)),
            pltpu.SemaphoreType.REGULAR,
            dma((COUNT,)),
            dma((COUNT,)),
            dma((COUNT,)),
            dma((COUNT,)),
            dma,
            dma,
        ],
        compiler_params=pltpu.CompilerParams(collective_id=0, has_side_effects=True, vmem_limit_bytes=12 * 1024 * 1024),
    )(*[pltpu.with_memory_space_constraint(v, pltpu.HBM) for v in (spins, kicks, stiffness)])
    def finish(final, energy, out, energy_out, sem):
        copies = [pltpu.make_async_copy(final, out, sem.at[0]), pltpu.make_async_copy(energy, energy_out, sem.at[1])]
        for copy in copies:
            copy.start()
        for copy in copies:
            copy.wait()

    final, energy = [pltpu.with_memory_space_constraint(v, pltpu.VMEM) for v in (final, energy)]
    return pl.pallas_call(
        finish,
        out_shape=(jax.ShapeDtypeStruct((2, NZ, NY, NX), F32), jax.ShapeDtypeStruct((16,), F32)),
        in_specs=[hbm, hbm],
        out_specs=(hbm, hbm),
        scratch_shapes=[dma((2,))],
        compiler_params=pltpu.CompilerParams(vmem_limit_bytes=1024 * 1024),
    )(final, energy)


def solution(mesh):
    dims = tuple(mesh.shape[a] for a in ("gz", "gy", "gx"))
    return jax.shard_map(
        functools.partial(body, dims),
        mesh=mesh,
        in_specs=(P(None, "gz", "gy", "gx"), P(None, None, "gz", "gy", "gx"), P("gz", "gy", "gx")),
        out_specs=(P(None, "gz", "gy", "gx"), P()),
        check_vma=False,
    )
```
